256 devices in a mesh: rows: 64 (over z, y, core), mem: 4 (over x).
Axes of the slice: x: 4, y: 4, z: 8, core: 2. Of those that a mesh axis runs over, the one named last changes fastest.
Arguments:
- control: bfloat16 [16, 32, 2, 512, 512], P('mem', None, None, 'rows'), may hold values from -6 to 6
- vert_root: float32 [32, 32], replicated, may hold values from -1 to 1
- loc_spec: float32 [512], replicated, may hold values from 0.1 to 1
- legendre: bfloat16 [512, 512, 768], P('rows'), as said below
- wave_table: int32 [512], replicated, may hold values from 0 to 511, as said below
- lat_order: int32 [768], replicated, may hold values from 0 to 767, each once
- perturb: bfloat16 [768, 16, 32, 1536], P('rows', None, 'mem'), may hold values from -3 to 3
Outputs:
- increment: bfloat16 [768, 32, 1536], P('rows', 'mem')
The draws below stay inside these ranges and needn't reach their ends.
Inputs may be any that keep to these rules, and one draw needn't show every extreme that they name: `wave_table`: every zonal wavenumber 0 to 511 sits in exactly one slot; the slots held by one index of rows are pairs m and 511 - m. legendre[s, n, t] is zero where n < wave_table[s]. `lat_order`: a permutation.
All inputs are finite; a program needn't handle non-finite values.
Results may differ from the reference program's by a relative error of at most 0.0085.
Values may be sent and summed in bfloat16 or wider, within the bound.
A program may use at most 128 MiB of HBM per device.

```python
import math
import jax
import jax.numpy as jnp
from jax import lax

NM = 512
NT = 512
NLAT = 768
NLON = 1536
MEMBERS = 16
LEV = 32
N_ROWS = 64


def pair_table(key):
    subkey = jax.random.fold_in(key, 7)
    permuted = jax.random.permutation(subkey, NM // 2).astype(jnp.int32)
    lower_half = permuted.reshape(N_ROWS, NM // (2 * N_ROWS))
    return jnp.concatenate([lower_half, NM - 1 - lower_half], axis=1).reshape(NM).astype(jnp.int32)


def draw_wave_table(key, part):
    return pair_table(key)


def draw_legendre(key, part):
    table = pair_table(key)
    subkey = jax.random.fold_in(key, 11)
    values = jax.random.normal(subkey, (NM, NT, NLAT), jnp.float32)
    totals = jnp.arange(NT, dtype=jnp.int32)
    triangle = (totals[None, :] >= table[:, None]).astype(jnp.float32)
    factor = (4.0 * NM * NT) ** (-0.5)
    return (values * factor * triangle[:, :, None]).astype(jnp.bfloat16)


def block_levels(key, extent, split, low, top_value):
    level = 1.0
    for dim, shards_of in split:
        draws = jax.random.uniform(jax.random.fold_in(jax.random.fold_in(key, 6), dim), (shards_of,), jnp.float32, low / len(split), top_value / len(split))
        level = level * jnp.repeat(jnp.exp(draws), extent[dim] // shards_of).reshape((-1,) + (1,) * (len(extent) - 1 - dim))
    return level


def noise(rng, dims, spread, reach, pieces=(), held_as=jnp.bfloat16):
    gain = block_levels(rng, dims, pieces, -0.22, 0.18) if pieces else 1.0
    values = jax.random.normal(rng, dims, jnp.float32) * spread * gain
    return jnp.minimum(jnp.maximum(values, -reach), reach).astype(held_as)


def setup_inputs(seed: int = 0) -> dict:
    key_list = jax.random.split(jax.random.key(seed), 8)
    control = noise(key_list[0], (MEMBERS, LEV, 2, NM, NT), 1.0, 6.0, ((0, 4), (3, 64)))
    vert_root = noise(key_list[1], (LEV, LEV), LEV ** -0.5, 1.0, (), jnp.float32)
    loc_spec = jnp.clip(jnp.exp(jax.random.uniform(key_list[2], (NT,), jnp.float32, math.log(0.1), math.log(1.0))), 0.1, 1.0)
    legendre = draw_legendre(jax.random.fold_in(key_list[7], 71), 0)
    wave_table = draw_wave_table(jax.random.fold_in(key_list[7], 71), 0)
    lat_order = jax.random.permutation(key_list[5], NLAT).astype(jnp.int32)
    perturb = noise(key_list[6], (NLAT, MEMBERS, LEV, NLON), 0.5, 3.0, ((0, 64), (2, 4)))
    return {"control": control, "vert_root": vert_root, "loc_spec": loc_spec, "legendre": legendre, "wave_table": wave_table, "lat_order": lat_order, "perturb": perturb}


def make_basis(wave_table, lon_count):
    longitude = lax.iota(jnp.int32, lon_count)
    phases = (wave_table[:, None] * longitude[None, :]) % lon_count
    angles = phases.astype(jnp.float32) * (2.0 * math.pi / lon_count)
    weights = jnp.where(wave_table == 0, 1.0, 2.0).astype(jnp.float32)[:, None]
    return jnp.stack([weights * jnp.cos(angles), -weights * jnp.sin(angles)]).astype(jnp.bfloat16)


def reference(control, vert_root, loc_spec, legendre, wave_table, lat_order, perturb):
    scaled = control.astype(jnp.float32) * loc_spec
    spectra = jnp.einsum('lv,kvrsn->klrsn', vert_root, scaled, precision=lax.Precision.HIGHEST).astype(jnp.bfloat16)
    zonal_basis = make_basis(wave_table, NLON).astype(jnp.float32)
    legendre_wide = legendre.astype(jnp.float32)

    def one_level(level_index):
        level_spec = lax.dynamic_index_in_dim(spectra, level_index, 1, keepdims=False).astype(jnp.float32)
        fourier = jnp.einsum('snt,krsn->strk', legendre_wide, level_spec, precision=lax.Precision.HIGHEST).astype(jnp.bfloat16)
        fourier = jnp.take(fourier, lat_order, axis=1).astype(jnp.float32)
        fields = jnp.einsum('sjrk,rsx->jkx', fourier, zonal_basis, precision=lax.Precision.HIGHEST).astype(jnp.bfloat16)
        member_ptb = lax.dynamic_index_in_dim(perturb, level_index, 2, keepdims=False).astype(jnp.float32)
        return jnp.sum(fields.astype(jnp.float32) * member_ptb, axis=1).astype(jnp.bfloat16)

    stacked = lax.map(one_level, jnp.arange(LEV, dtype=jnp.int32))
    return jnp.transpose(stacked, (1, 0, 2))
```

```python
import functools
import math

import jax
import jax.numpy as jnp
from jax import lax
from jax.experimental import pallas as pl
from jax.experimental.pallas import tpu as pltpu
from jax.sharding import PartitionSpec as P

MESH = pl.DeviceIdType.MESH
F32, BF16 = jnp.float32, jnp.bfloat16
NT_DIMS = (((1,), (1,)), ((), ()))


def dot(a, b):
    return jnp.dot(a, b, preferred_element_type=F32)


def split3(a):
    hi = a.astype(BF16)
    rest = a - hi.astype(F32)
    mid = rest.astype(BF16)
    low = (rest - mid.astype(F32)).astype(BF16)
    return hi, mid, low


def spread_rows(row):
    return jnp.transpose(jnp.broadcast_to(row, (128, 128)))


def peer(row, mem, o):
    z, y, c = lax.div(row, 8), lax.rem(lax.div(row, 2), 4), lax.rem(row, 2)
    z = lax.rem(z + lax.div(o, 32), 8)
    y = lax.rem(y + lax.rem(lax.div(o, 8), 4), 4)
    c = lax.rem(c + lax.rem(lax.div(o, 4), 2), 2)
    return (z * 4 + y) * 2 + c, lax.rem(mem + lax.rem(o, 4), 4)


def kernel(
    control, root, loc, legendre, waves, order, perturb, out,
    ctrl, leg, pert, sp32, spec, four, latf, onehot, msg, snd, rcv, wavef, basis, lhs,
    in_sem, leg_sem, send_sem, recv_sem,
):
    row, mem = lax.axis_index("rows"), lax.axis_index("mem")
    barrier = pltpu.get_barrier_semaphore()

    for k in range(4):
        pltpu.make_async_copy(control.at[k], ctrl.at[k], in_sem.at[k]).start()

    def load_leg(s, _):
        pltpu.make_async_copy(legendre.at[s], leg.at[s], leg_sem.at[s]).start()
        return 0

    lax.fori_loop(0, 8, load_leg, 0)
    pltpu.make_async_copy(perturb, pert, in_sem.at[4]).start()

    def greet(o, _):
        r, m = peer(row, mem, o)
        pl.semaphore_signal(barrier, inc=1, device_id=(r, m), device_id_type=MESH)
        return 0

    lax.fori_loop(1, 256, greet, 0)

    pick = (
        lax.broadcasted_iota(jnp.int32, (256, 32), 0) % 32
        == lax.broadcasted_iota(jnp.int32, (256, 32), 1)
    ).astype(F32).astype(BF16)
    widen = (
        lax.broadcasted_iota(jnp.int32, (32, 256), 1) // 8
        == lax.broadcasted_iota(jnp.int32, (32, 256), 0)
    ).astype(F32).astype(BF16)
    same = (
        lax.broadcasted_iota(jnp.int32, (256, 256), 0) // 32
        == lax.broadcasted_iota(jnp.int32, (256, 256), 1) % 8
    )
    mix = [
        jnp.where(same, dot(dot(pick, part).astype(BF16), widen), 0.0).astype(BF16)
        for part in split3(root[...])
    ]

    for b in range(6):
        latf[b * 128:(b + 1) * 128, :] = spread_rows(order[b:b + 1, :].astype(F32))
    lane = lax.broadcasted_iota(jnp.int32, (64, 128), 1)
    lane_f = lane.astype(F32)
    for c in range(3):
        for q in range(4):
            rows = latf[pl.ds(c * 4 + q, 64, stride=12), :]
            for b in range(6):
                hit = rows == lane_f + float(b * 128)
                onehot[c, q * 64:(q + 1) * 64, b * 128:(b + 1) * 128] = jnp.where(
                    hit, 1.0, 0.0
                ).astype(BF16)

    for k in range(4):
        pltpu.make_async_copy(control.at[k], ctrl.at[k], in_sem.at[k]).wait()
    scale = loc[...]
    for r in range(2):
        for k in range(4):
            x = ctrl[k, :, r].reshape(256, 512)
            mixed = (dot(mix[0], x) + dot(mix[1], x) + dot(mix[2], x)) * scale
            sp32[:, :, k] = mixed.reshape(8, 4, 8, 512)

        def narrow(s, _):
            spec[s, r * 128:(r + 1) * 128, :] = sp32[s].reshape(128, 512).astype(BF16)
            return 0

        lax.fori_loop(0, 8, narrow, 0)

    def transform(s, _):
        pltpu.make_async_copy(legendre.at[s], leg.at[s], leg_sem.at[s]).wait()
        four[s] = dot(spec[s], leg[s]).astype(BF16)
        return 0

    lax.fori_loop(0, 8, transform, 0)

    group = lane // 32
    me = mem * 64 + row
    pl.semaphore_wait(barrier, 255)

    def build(c, _):
        def one(s, _):
            picked = lax.dot_general(onehot[c], four[s], NT_DIMS, preferred_element_type=F32)
            for r in range(2):
                rolled = []
                for q in range(4):
                    part = picked[q * 64:(q + 1) * 64, r * 128:(r + 1) * 128]
                    rolled.append(pltpu.roll(part, q * 32, 1) if q else part)
                for level in range(4):
                    tile = rolled[(0 - level) % 4]
                    for g in range(1, 4):
                        tile = jnp.where(group == g, rolled[(g - level) % 4], tile)
                    msg[pl.ds(level * 16 + r * 8 + s, 64, stride=64), :] = tile
            return 0

        lax.fori_loop(0, 8, one, 0)

        def pack(b, _):
            start = pl.multiple_of(b * 512, 512)
            snd[c, pl.ds(b * 32, 32)] = msg[pl.ds(start, 512), :].reshape(32, 16, 128).astype(BF16)
            return 0

        lax.fori_loop(0, 8, pack, 0)

        def send(o, _):
            r, m = peer(row, mem, o)
            pltpu.make_async_remote_copy(
                src_ref=snd.at[c, r * 4 + m],
                dst_ref=rcv.at[c, me],
                send_sem=send_sem.at[c],
                recv_sem=recv_sem.at[c],
                device_id=(r, m),
                device_id_type=MESH,
            ).start()
            return 0

        lax.fori_loop(1, 256, send, 0)
        rcv[c, me] = snd[c, row * 4 + mem]
        return 0

    lax.fori_loop(0, 3, build, 0)

    for b in range(4):
        wavef[b * 128:(b + 1) * 128, :] = spread_rows(waves[b:b + 1, :].astype(F32))

    def angles(wave, step):
        phase = wave * step
        phase = phase - 1536.0 * jnp.floor(phase * (1.0 / 1536.0))
        return phase * (2.0 * math.pi / 1536.0)

    def make_basis(b, _):
        wave = wavef[pl.ds(pl.multiple_of(b * 64, 64), 64), :]
        weight = jnp.where(wave == 0.0, 1.0, 2.0)
        near = angles(wave, lane_f)
        far = angles(wave, 128.0)
        cos, sin = weight * jnp.cos(near), weight * jnp.sin(near)
        turn_cos, turn_sin = jnp.cos(far), jnp.sin(far)
        for a in range(12):
            pair = jnp.stack([cos.reshape(8, 8, 128), -sin.reshape(8, 8, 128)], axis=1)
            basis[pl.ds(pl.multiple_of(b * 128, 128), 128), a * 128:(a + 1) * 128] = (
                pair.reshape(128, 128).astype(BF16)
            )
            cos, sin = cos * turn_cos - sin * turn_sin, sin * turn_cos + cos * turn_sin
        return 0

    lax.fori_loop(0, 8, make_basis, 0)
    pltpu.make_async_copy(perturb, pert, in_sem.at[4]).wait()

    def finish(c, _):
        pltpu.make_async_copy(
            rcv.at[c, pl.ds(0, 255)], rcv.at[c, pl.ds(0, 255)], recv_sem.at[c]
        ).wait()
        for kg in range(4):
            lhs[kg * 128:(kg + 1) * 128, :] = jnp.transpose(
                rcv[c, kg * 64:(kg + 1) * 64].reshape(1024, 128)
            )

        def columns(n, _):
            cols = pl.ds(pl.multiple_of(n * 256, 256), 256)
            field = dot(lhs[...], basis[:, cols]).astype(BF16).astype(F32)
            field = field.reshape(4, 4, 4, 8, 256)
            for g in range(4):
                j = c * 4 + lax.rem(g + 4 - mem, 4)
                weights = pert[j, :, :, cols].astype(F32).reshape(4, 4, 8, 256)
                out[j, :, cols] = jnp.sum(field[:, g] * weights, axis=(0, 1)).astype(BF16)
            return 0

        lax.fori_loop(0, 6, columns, 0)
        pltpu.make_async_copy(
            snd.at[c, pl.ds(0, 255)], snd.at[c, pl.ds(0, 255)], send_sem.at[c]
        ).wait()
        return 0

    lax.fori_loop(0, 3, finish, 0)


def shards(control, vert_root, loc_spec, legendre, wave_table, lat_order, perturb):
    vmem = pl.BlockSpec(memory_space=pltpu.VMEM)
    hbm = pl.BlockSpec(memory_space=pl.ANY)
    return pl.pallas_call(
        kernel,
        name="synthesis",
        out_shape=jax.ShapeDtypeStruct((12, 8, 1536), BF16),
        in_specs=[hbm, vmem, vmem, hbm, vmem, vmem, hbm],
        out_specs=vmem,
        scratch_shapes=[
            pltpu.VMEM((4, 32, 2, 8, 512), BF16),
            pltpu.VMEM((8, 512, 768), BF16),
            pltpu.VMEM((12, 16, 8, 1536), BF16),
            pltpu.VMEM((8, 4, 4, 8, 512), F32),
            pltpu.VMEM((8, 256, 512), BF16),
            pltpu.VMEM((8, 256, 768), BF16),
            pltpu.VMEM((768, 128), F32),
            pltpu.VMEM((3, 256, 768), BF16),
            pltpu.VMEM((4096, 128), F32),
            pltpu.VMEM((3, 256, 16, 128), BF16),
            pltpu.VMEM((3, 256, 16, 128), BF16),
            pltpu.VMEM((512, 128), F32),
            pltpu.VMEM((1024, 1536), BF16),
            pltpu.VMEM((512, 1024), BF16),
            pltpu.SemaphoreType.DMA((5,)),
            pltpu.SemaphoreType.DMA((8,)),
            pltpu.SemaphoreType.DMA((3,)),
            pltpu.SemaphoreType.DMA((3,)),
        ],
        compiler_params=pltpu.CompilerParams(
            collective_id=0, has_side_effects=True, vmem_limit_bytes=60 * 1024 * 1024
        ),
    )(
        control, vert_root, loc_spec.reshape(1, 512), legendre,
        wave_table.reshape(4, 128), lat_order.reshape(6, 128), perturb,
    )


def solution(mesh):
    return jax.shard_map(
        shards,
        mesh=mesh,
        in_specs=(
            P("mem", None, None, "rows", None),
            P(),
            P(),
            P("rows", None, None),
            P(),
            P(),
            P("rows", None, "mem", None),
        ),
        out_specs=P("rows", "mem", None),
        check_vma=False,
    )
```

```python
import functools
import math

import jax
import jax.numpy as jnp
from jax import lax
from jax.experimental import pallas as pl
from jax.experimental.pallas import tpu as pltpu
from jax.sharding import PartitionSpec as P

MESH = pl.DeviceIdType.MESH
F32, BF16 = jnp.float32, jnp.bfloat16
NT_DIMS = (((1,), (1,)), ((), ()))


def dot(a, b):
    return jnp.dot(a, b, preferred_element_type=F32)


def split2(a):
    hi = a.astype(BF16)
    return hi, (a - hi.astype(F32)).astype(BF16)


def spread_rows(row):
    return jnp.transpose(jnp.broadcast_to(row, (128, 128)))


def everyone_else(row, mem, act):
    mems = [mem] + [lax.rem(mem + d, 4) for d in range(1, 4)]
    for d in range(1, 4):
        act(row, mems[d])

    def whole_row(r, _):
        for m in mems:
            act(r, m)
        return 0

    lax.fori_loop(row + 1, 64, whole_row, 0)
    lax.fori_loop(0, row, whole_row, 0)


def kernel(
    control, root, loc, legendre, waves, order, perturb, out,
    ctrl, leg, pert, sp32, spec, four, latf, onehot, msg, snd, rcv, wavef, basis, lhs,
    in_sem, leg_sem, send_sem, recv_sem,
):
    row, mem = lax.axis_index("rows"), lax.axis_index("mem")
    barrier = pltpu.get_barrier_semaphore()

    for k in range(4):
        pltpu.make_async_copy(control.at[k], ctrl.at[k], in_sem.at[k]).start()

    def greet(r, m):
        pl.semaphore_signal(barrier, inc=1, device_id=(r, m), device_id_type=MESH)

    everyone_else(row, mem, greet)
    for s in range(8):
        pltpu.make_async_copy(legendre.at[s], leg.at[s], leg_sem.at[s]).start()

    pick = (
        lax.broadcasted_iota(jnp.int32, (256, 32), 0) % 32
        == lax.broadcasted_iota(jnp.int32, (256, 32), 1)
    ).astype(F32).astype(BF16)
    widen = (
        lax.broadcasted_iota(jnp.int32, (32, 256), 1) // 8
        == lax.broadcasted_iota(jnp.int32, (32, 256), 0)
    ).astype(F32).astype(BF16)
    same = (
        lax.broadcasted_iota(jnp.int32, (256, 256), 0) // 32
        == lax.broadcasted_iota(jnp.int32, (256, 256), 1) % 8
    )
    mix = [
        jnp.where(same, dot(dot(pick, part).astype(BF16), widen), 0.0).astype(BF16)
        for part in split2(root[...])
    ]

    for b in range(6):
        latf[b * 128:(b + 1) * 128, :] = spread_rows(order[b:b + 1, :].astype(F32))
    lane = lax.broadcasted_iota(jnp.int32, (64, 128), 1)
    lane_f = lane.astype(F32)
    for c in range(3):
        for q in range(4):
            rows = latf[pl.ds(c * 4 + q, 64, stride=12), :]
            for b in range(6):
                hit = rows == lane_f + float(b * 128)
                onehot[c, q * 64:(q + 1) * 64, b * 128:(b + 1) * 128] = jnp.where(
                    hit, 1.0, 0.0
                ).astype(BF16)

    for k in range(4):
        pltpu.make_async_copy(control.at[k], ctrl.at[k], in_sem.at[k]).wait()
    scale = loc[...]
    for r in range(2):
        for k in range(4):
            x = ctrl[k, :, r].reshape(256, 512)
            mixed = (dot(mix[0], x) + dot(mix[1], x)) * scale
            sp32[:, :, k] = mixed.reshape(8, 4, 8, 512)

        def narrow(s, _):
            spec[s, r * 128:(r + 1) * 128, :] = sp32[s].reshape(128, 512).astype(BF16)
            return 0

        lax.fori_loop(0, 8, narrow, 0)

    def transform(s, _):
        pltpu.make_async_copy(legendre.at[s], leg.at[s], leg_sem.at[s]).wait()
        four[s] = dot(spec[s], leg[s]).astype(BF16)
        return 0

    lax.fori_loop(0, 8, transform, 0)

    pltpu.make_async_copy(perturb, pert, in_sem.at[4]).start()
    group = lane // 32
    me = mem * 64 + row
    pl.semaphore_wait(barrier, 255)

    def build(c, _):
        def some(i, _):
            for s in (i * 4, i * 4 + 1, i * 4 + 2, i * 4 + 3):
                picked = lax.dot_general(onehot[c], four[s], NT_DIMS, preferred_element_type=F32)
                for r in range(2):
                    rolled = []
                    for q in range(4):
                        part = picked[q * 64:(q + 1) * 64, r * 128:(r + 1) * 128]
                        rolled.append(pltpu.roll(part, q * 32, 1) if q else part)
                    for level in range(4):
                        tile = rolled[(0 - level) % 4]
                        for g in range(1, 4):
                            tile = jnp.where(group == g, rolled[(g - level) % 4], tile)
                        msg[pl.ds(level * 16 + r * 8 + s, 64, stride=72), :] = tile
            return 0

        lax.fori_loop(0, 2, some, 0)

        def pack(b, _):
            for j in range(8):
                start = pl.multiple_of((b * 8 + j) * 72, 8)
                snd[c, pl.ds(b * 32 + j * 4, 4)] = (
                    msg[pl.ds(start, 64), :].reshape(4, 16, 128).astype(BF16)
                )
            return 0

        lax.fori_loop(0, 8, pack, 0)

        def send(r, m):
            pltpu.make_async_remote_copy(
                src_ref=snd.at[c, r * 4 + m],
                dst_ref=rcv.at[c, me],
                send_sem=send_sem.at[c],
                recv_sem=recv_sem.at[c],
                device_id=(r, m),
                device_id_type=MESH,
            ).start()

        everyone_else(row, mem, send)
        rcv[c, me] = snd[c, row * 4 + mem]
        return 0

    lax.fori_loop(0, 3, build, 0)

    for b in range(4):
        wavef[b * 128:(b + 1) * 128, :] = spread_rows(waves[b:b + 1, :].astype(F32))

    def angles(wave, step):
        phase = wave * step
        phase = phase - 1536.0 * jnp.floor(phase * (1.0 / 1536.0))
        return phase * (2.0 * math.pi / 1536.0)

    def make_basis(b, _):
        wave = wavef[pl.ds(pl.multiple_of(b * 64, 64), 64), :]
        weight = jnp.where(wave == 0.0, 1.0, 2.0)
        near = angles(wave, lane_f)
        far = angles(wave, 128.0)
        cos, sin = weight * jnp.cos(near), weight * jnp.sin(near)
        turn_cos, turn_sin = jnp.cos(far), jnp.sin(far)
        for a in range(12):
            pair = jnp.stack([cos.reshape(8, 8, 128), -sin.reshape(8, 8, 128)], axis=1)
            basis[pl.ds(pl.multiple_of(b * 128, 128), 128), a * 128:(a + 1) * 128] = (
                pair.reshape(128, 128).astype(BF16)
            )
            cos, sin = cos * turn_cos - sin * turn_sin, sin * turn_cos + cos * turn_sin
        return 0

    lax.fori_loop(0, 8, make_basis, 0)
    pltpu.make_async_copy(perturb, pert, in_sem.at[4]).wait()

    def finish(c, _):
        pltpu.make_async_copy(
            rcv.at[c, pl.ds(0, 255)], rcv.at[c, pl.ds(0, 255)], recv_sem.at[c]
        ).wait()
        for kg in range(4):
            lhs[kg * 128:(kg + 1) * 128, :] = jnp.transpose(
                rcv[c, kg * 64:(kg + 1) * 64].reshape(1024, 128)
            )

        def columns(n, _):
            cols = pl.ds(pl.multiple_of(n * 256, 256), 256)
            field = dot(lhs[...], basis[:, cols]).astype(BF16).astype(F32)
            field = field.reshape(4, 4, 4, 8, 256)
            for g in range(4):
                j = c * 4 + lax.rem(g + 4 - mem, 4)
                weights = pert[j, :, :, cols].astype(F32).reshape(4, 4, 8, 256)
                out[j, :, cols] = jnp.sum(field[:, g] * weights, axis=(0, 1)).astype(BF16)
            return 0

        lax.fori_loop(0, 6, columns, 0)
        pltpu.make_async_copy(
            snd.at[c, pl.ds(0, 255)], snd.at[c, pl.ds(0, 255)], send_sem.at[c]
        ).wait()
        return 0

    lax.fori_loop(0, 3, finish, 0)


def shards(control, vert_root, loc_spec, legendre, wave_table, lat_order, perturb):
    vmem = pl.BlockSpec(memory_space=pltpu.VMEM)
    hbm = pl.BlockSpec(memory_space=pl.ANY)
    return pl.pallas_call(
        kernel,
        name="synthesis",
        out_shape=jax.ShapeDtypeStruct((12, 8, 1536), BF16),
        in_specs=[hbm, vmem, vmem, hbm, vmem, vmem, hbm],
        out_specs=vmem,
        scratch_shapes=[
            pltpu.VMEM((4, 32, 2, 8, 512), BF16),
            pltpu.VMEM((8, 512, 768), BF16),
            pltpu.VMEM((12, 16, 8, 1536), BF16),
            pltpu.VMEM((8, 4, 4, 8, 512), F32),
            pltpu.VMEM((8, 256, 512), BF16),
            pltpu.VMEM((8, 256, 768), BF16),
            pltpu.VMEM((768, 128), F32),
            pltpu.VMEM((3, 256, 768), BF16),
            pltpu.VMEM((64 * 72, 128), F32),
            pltpu.VMEM((3, 256, 16, 128), BF16),
            pltpu.VMEM((3, 256, 16, 128), BF16),
            pltpu.VMEM((512, 128), F32),
            pltpu.VMEM((1024, 1536), BF16),
            pltpu.VMEM((512, 1024), BF16),
            pltpu.SemaphoreType.DMA((5,)),
            pltpu.SemaphoreType.DMA((8,)),
            pltpu.SemaphoreType.DMA((3,)),
            pltpu.SemaphoreType.DMA((3,)),
        ],
        compiler_params=pltpu.CompilerParams(
            collective_id=0, has_side_effects=True, vmem_limit_bytes=60 * 1024 * 1024
        ),
    )(
        control, vert_root, loc_spec.reshape(1, 512), legendre,
        wave_table.reshape(4, 128), lat_order.reshape(6, 128), perturb,
    )


def solution(mesh):
    return jax.shard_map(
        shards,
        mesh=mesh,
        in_specs=(
            P("mem", None, None, "rows", None),
            P(),
            P(),
            P("rows", None, None),
            P(),
            P(),
            P("rows", None, "mem", None),
        ),
        out_specs=P("rows", "mem", None),
        check_vma=False,
    )
```

```python
import functools
import math

import jax
import jax.numpy as jnp
from jax import lax
from jax.experimental import pallas as pl
from jax.experimental.pallas import tpu as pltpu
from jax.sharding import PartitionSpec as P

MESH = pl.DeviceIdType.MESH
F32, BF16 = jnp.float32, jnp.bfloat16
NT_DIMS = (((1,), (1,)), ((), ()))


def dot(a, b):
    return jnp.dot(a, b, preferred_element_type=F32)


def split2(a):
    hi = a.astype(BF16)
    return hi, (a - hi.astype(F32)).astype(BF16)


def spread_rows(row):
    return jnp.transpose(jnp.broadcast_to(row, (128, 128)))


def everyone_else(row, mem, act):
    mems = [mem] + [lax.rem(mem + d, 4) for d in range(1, 4)]
    for d in range(1, 4):
        act(row, mems[d])

    def whole_row(r, _):
        for m in mems:
            act(r, m)
        return 0

    lax.fori_loop(row + 1, 64, whole_row, 0)
    lax.fori_loop(0, row, whole_row, 0)


def far_first(row, mem, act):
    z, y, c = lax.div(row, 8), lax.rem(lax.div(row, 2), 4), lax.rem(row, 2)
    planes = [lax.rem(z + dz, 8) * 8 for dz in (4, 3, 5, 2, 6, 1, 7, 0)]
    cores = [1 - c, c]
    for dx in (2, 1, 3, 0):
        m = lax.rem(mem + dx, 4)

        def at(dy, skip, m=m):
            line = lax.rem(y + dy, 4) * 2
            for i, core in enumerate(cores):
                for j, plane in enumerate(planes):
                    if not (skip and i == 1 and j == 7):
                        act(plane + line + core, m)

        def step(t, _, at=at):
            at(3 - t, False)
            return 0

        lax.fori_loop(0, 4 if dx else 3, step, 0)
        if not dx:
            at(0, True)


def kernel(
    control, root_in, loc_in, legendre, waves_in, order_in, perturb, out_hbm,
    root, loc, waves, order, out,
    ctrl, leg, pert, sp32, spec, four, latf, onehot, msg, snd, rcv, wavef, basis, lhs, total,
    in_sem, leg_sem, small_sem, out_sem, send_sem, recv_sem,
):
    row, mem = lax.axis_index("rows"), lax.axis_index("mem")
    barrier = pltpu.get_barrier_semaphore()

    small = [
        pltpu.make_async_copy(src, dst, small_sem.at[i])
        for i, (src, dst) in enumerate(
            ((root_in, root), (order_in, order), (loc_in, loc), (waves_in, waves))
        )
    ]
    small[0].start()
    for k in range(4):
        pltpu.make_async_copy(control.at[k], ctrl.at[k], in_sem.at[k]).start()
    for copy in small[1:]:
        copy.start()

    def greet(r, m):
        pl.semaphore_signal(barrier, inc=1, device_id=(r, m), device_id_type=MESH)

    everyone_else(row, mem, greet)
    for s in range(8):
        pltpu.make_async_copy(legendre.at[s], leg.at[s], leg_sem.at[s]).start()

    pick = (
        lax.broadcasted_iota(jnp.int32, (256, 32), 0) % 32
        == lax.broadcasted_iota(jnp.int32, (256, 32), 1)
    ).astype(F32).astype(BF16)
    widen = (
        lax.broadcasted_iota(jnp.int32, (32, 256), 1) // 8
        == lax.broadcasted_iota(jnp.int32, (32, 256), 0)
    ).astype(F32).astype(BF16)
    same = (
        lax.broadcasted_iota(jnp.int32, (256, 256), 0) // 32
        == lax.broadcasted_iota(jnp.int32, (256, 256), 1) % 8
    )
    small[0].wait()
    mix = [
        jnp.where(same, dot(dot(pick, part).astype(BF16), widen), 0.0).astype(BF16)
        for part in split2(root[...])
    ]

    small[1].wait()
    for b in range(6):
        latf[b * 128:(b + 1) * 128, :] = spread_rows(order[b:b + 1, :].astype(F32))
    lane = lax.broadcasted_iota(jnp.int32, (64, 128), 1)
    lane_f = lane.astype(F32)
    for c in range(3):
        for q in range(4):
            rows = latf[pl.ds(c * 4 + q, 64, stride=12), :]
            for b in range(6):
                hit = rows == lane_f + float(b * 128)
                onehot[c, q * 64:(q + 1) * 64, b * 128:(b + 1) * 128] = jnp.where(
                    hit, 1.0, 0.0
                ).astype(BF16)

    for k in range(4):
        pltpu.make_async_copy(control.at[k], ctrl.at[k], in_sem.at[k]).wait()
    small[2].wait()
    scale = loc[...]
    for r in range(2):
        for k in range(4):
            x = ctrl[k, :, r].reshape(256, 512)
            mixed = (dot(mix[0], x) + dot(mix[1], x)) * scale
            sp32[:, :, k] = mixed.reshape(8, 4, 8, 512)

        def narrow(s, _):
            spec[s, r * 128:(r + 1) * 128, :] = sp32[s].reshape(128, 512).astype(BF16)
            return 0

        lax.fori_loop(0, 8, narrow, 0)

    def transform(s, _):
        pltpu.make_async_copy(legendre.at[s], leg.at[s], leg_sem.at[s]).wait()
        four[s] = dot(spec[s], leg[s]).astype(BF16)
        return 0

    lax.fori_loop(0, 8, transform, 0)

    pltpu.make_async_copy(perturb, pert, in_sem.at[4]).start()
    group = lane // 32
    me = mem * 64 + row
    pl.semaphore_wait(barrier, 255)

    def build(c, _):
        def some(i, _):
            for s in (i * 4, i * 4 + 1, i * 4 + 2, i * 4 + 3):
                picked = lax.dot_general(onehot[c], four[s], NT_DIMS, preferred_element_type=F32)
                for r in range(2):
                    rolled = []
                    for q in range(4):
                        part = picked[q * 64:(q + 1) * 64, r * 128:(r + 1) * 128]
                        rolled.append(pltpu.roll(part, q * 32, 1) if q else part)
                    for level in range(4):
                        tile = rolled[(0 - level) % 4]
                        for g in range(1, 4):
                            tile = jnp.where(group == g, rolled[(g - level) % 4], tile)
                        msg[pl.ds(level * 16 + r * 8 + s, 64, stride=72), :] = tile
            return 0

        lax.fori_loop(0, 2, some, 0)

        def pack(b, _):
            for j in range(8):
                start = pl.multiple_of((b * 8 + j) * 72, 8)
                snd[c, pl.ds(b * 32 + j * 4, 4)] = (
                    msg[pl.ds(start, 64), :].reshape(4, 16, 128).astype(BF16)
                )
            return 0

        lax.fori_loop(0, 8, pack, 0)

        def send(r, m):
            pltpu.make_async_remote_copy(
                src_ref=snd.at[c, r * 4 + m],
                dst_ref=rcv.at[c, me],
                send_sem=send_sem.at[c],
                recv_sem=recv_sem.at[c, mem],
                device_id=(r, m),
                device_id_type=MESH,
            ).start()

        far_first(row, mem, send)
        rcv[c, me] = snd[c, row * 4 + mem]
        return 0

    lax.fori_loop(0, 3, build, 0)

    small[3].wait()
    for b in range(4):
        wavef[b * 128:(b + 1) * 128, :] = spread_rows(waves[b:b + 1, :].astype(F32))

    def angles(wave, step):
        phase = wave * step
        phase = phase - 1536.0 * jnp.floor(phase * (1.0 / 1536.0))
        return phase * (2.0 * math.pi / 1536.0)

    def make_basis(b, _):
        wave = wavef[pl.ds(pl.multiple_of(b * 64, 64), 64), :]
        weight = jnp.where(wave == 0.0, 1.0, 2.0)
        near = angles(wave, lane_f)
        far = angles(wave, 128.0)
        cos, sin = weight * jnp.cos(near), weight * jnp.sin(near)
        turn_cos, turn_sin = jnp.cos(far), jnp.sin(far)
        for a in range(12):
            pair = jnp.stack([cos.reshape(8, 8, 128), -sin.reshape(8, 8, 128)], axis=1)
            basis[pl.ds(pl.multiple_of(b * 128, 128), 128), a * 128:(a + 1) * 128] = (
                pair.reshape(128, 128).astype(BF16)
            )
            cos, sin = cos * turn_cos - sin * turn_sin, sin * turn_cos + cos * turn_sin
        return 0

    lax.fori_loop(0, 8, make_basis, 0)
    pltpu.make_async_copy(perturb, pert, in_sem.at[4]).wait()

    def finish(c, _):
        for step, dx in enumerate((2, 1, 3, 0)):
            kg = lax.rem(mem + 4 - dx, 4)
            landed = rcv.at[c, pl.ds(0, 64 if dx else 63)]
            pltpu.make_async_copy(landed, landed, recv_sem.at[c, kg]).wait()
            lhs[...] = jnp.transpose(rcv[c, pl.ds(kg * 64, 64)].reshape(1024, 128))

            def columns(n, _, step=step, kg=kg):
                cols = pl.ds(pl.multiple_of(n * 256, 256), 256)
                field = dot(lhs[...], basis[:, cols]).astype(BF16).astype(F32)
                field = field.reshape(4, 4, 8, 256)
                for g in range(4):
                    j = c * 4 + lax.rem(g + 4 - mem, 4)
                    weights = pert[j, pl.ds(kg * 4, 4), :, cols].astype(F32)
                    part = jnp.sum(field[g] * weights, axis=0)
                    if step:
                        part = part + total[g, :, cols]
                    if step == 3:
                        out[j, :, cols] = part.astype(BF16)
                    else:
                        total[g, :, cols] = part
                return 0

            lax.fori_loop(0, 6, columns, 0)
        rows = pl.ds(c * 4, 4)
        pltpu.make_async_copy(out.at[rows], out_hbm.at[rows], out_sem.at[c]).start()
        pltpu.make_async_copy(
            snd.at[c, pl.ds(0, 255)], snd.at[c, pl.ds(0, 255)], send_sem.at[c]
        ).wait()
        return 0

    lax.fori_loop(0, 3, finish, 0)
    for c in range(3):
        rows = pl.ds(c * 4, 4)
        pltpu.make_async_copy(out.at[rows], out_hbm.at[rows], out_sem.at[c]).wait()


def shards(control, vert_root, loc_spec, legendre, wave_table, lat_order, perturb):
    hbm = pl.BlockSpec(memory_space=pl.ANY)
    return pl.pallas_call(
        kernel,
        name="synthesis",
        out_shape=jax.ShapeDtypeStruct((12, 8, 1536), BF16),
        in_specs=[hbm] * 7,
        out_specs=hbm,
        scratch_shapes=[
            pltpu.VMEM((32, 32), F32),
            pltpu.VMEM((1, 512), F32),
            pltpu.VMEM((4, 128), jnp.int32),
            pltpu.VMEM((6, 128), jnp.int32),
            pltpu.VMEM((12, 8, 1536), BF16),
            pltpu.VMEM((4, 32, 2, 8, 512), BF16),
            pltpu.VMEM((8, 512, 768), BF16),
            pltpu.VMEM((12, 16, 8, 1536), BF16),
            pltpu.VMEM((8, 4, 4, 8, 512), F32),
            pltpu.VMEM((8, 256, 512), BF16),
            pltpu.VMEM((8, 256, 768), BF16),
            pltpu.VMEM((768, 128), F32),
            pltpu.VMEM((3, 256, 768), BF16),
            pltpu.VMEM((64 * 72, 128), F32),
            pltpu.VMEM((3, 256, 16, 128), BF16),
            pltpu.VMEM((3, 256, 16, 128), BF16),
            pltpu.VMEM((512, 128), F32),
            pltpu.VMEM((1024, 1536), BF16),
            pltpu.VMEM((128, 1024), BF16),
            pltpu.VMEM((4, 8, 1536), F32),
            pltpu.SemaphoreType.DMA((5,)),
            pltpu.SemaphoreType.DMA((8,)),
            pltpu.SemaphoreType.DMA((4,)),
            pltpu.SemaphoreType.DMA((3,)),
            pltpu.SemaphoreType.DMA((3,)),
            pltpu.SemaphoreType.DMA((3, 4)),
        ],
        compiler_params=pltpu.CompilerParams(
            collective_id=0, has_side_effects=True, vmem_limit_bytes=60 * 1024 * 1024
        ),
    )(
        control, vert_root, loc_spec.reshape(1, 512), legendre,
        wave_table.reshape(4, 128), lat_order.reshape(6, 128), perturb,
    )


def solution(mesh):
    return jax.shard_map(
        shards,
        mesh=mesh,
        in_specs=(
            P("mem", None, None, "rows", None),
            P(),
            P(),
            P("rows", None, None),
            P(),
            P(),
            P("rows", None, "mem", None),
        ),
        out_specs=P("rows", "mem", None),
        check_vma=False,
    )
```

```python
import functools
import math

import jax
import jax.numpy as jnp
from jax import lax
from jax.experimental import pallas as pl
from jax.experimental.pallas import tpu as pltpu
from jax.sharding import PartitionSpec as P

MESH = pl.DeviceIdType.MESH
F32, BF16 = jnp.float32, jnp.bfloat16
NT_DIMS = (((1,), (1,)), ((), ()))


def dot(a, b):
    return jnp.dot(a, b, preferred_element_type=F32)


def split2(a):
    hi = a.astype(BF16)
    return hi, (a - hi.astype(F32)).astype(BF16)


def spread_rows(row):
    return jnp.transpose(jnp.broadcast_to(row, (128, 128)))


def everyone_else(row, mem, act):
    mems = [mem] + [lax.rem(mem + d, 4) for d in range(1, 4)]
    for d in range(1, 4):
        act(row, mems[d])

    def whole_row(r, _):
        for m in mems:
            act(r, m)
        return 0

    lax.fori_loop(row + 1, 64, whole_row, 0)
    lax.fori_loop(0, row, whole_row, 0)


def far_first(row, mem, act):
    z, y, c = lax.div(row, 8), lax.rem(lax.div(row, 2), 4), lax.rem(row, 2)
    planes = [lax.rem(z + dz, 8) * 8 for dz in (4, 3, 5, 2, 6, 1, 7, 0)]
    cores = [1 - c, c]
    for dx in (2, 1, 3, 0):
        m = lax.rem(mem + dx, 4)

        def at(dy, skip, m=m):
            line = lax.rem(y + dy, 4) * 2
            for i, core in enumerate(cores):
                for j, plane in enumerate(planes):
                    if not (skip and i == 1 and j == 7):
                        act(plane + line + core, m)

        def step(t, _, at=at):
            at(3 - t, False)
            return 0

        lax.fori_loop(0, 4 if dx else 3, step, 0)
        if not dx:
            at(0, True)


def kernel(
    control, root_in, loc_in, legendre, waves_in, order_in, perturb, out_hbm,
    root, loc, waves, order, out,
    ctrl, leg, pert, sp32, spec, four, latf, onehot, msg, snd, rcv, wavef, basis, lhs, total,
    in_sem, leg_sem, small_sem, out_sem, send_sem, recv_sem,
):
    row, mem = lax.axis_index("rows"), lax.axis_index("mem")
    barrier = pltpu.get_barrier_semaphore()

    small = [
        pltpu.make_async_copy(src, dst, small_sem.at[i])
        for i, (src, dst) in enumerate(
            ((root_in, root), (order_in, order), (loc_in, loc), (waves_in, waves))
        )
    ]
    small[0].start()
    for k in range(4):
        pltpu.make_async_copy(control.at[k], ctrl.at[k], in_sem.at[k]).start()
    for copy in small[1:]:
        copy.start()

    def greet(r, m):
        pl.semaphore_signal(barrier, inc=1, device_id=(r, m), device_id_type=MESH)

    everyone_else(row, mem, greet)
    for s in range(8):
        pltpu.make_async_copy(legendre.at[s], leg.at[s], leg_sem.at[s]).start()

    pick = (
        lax.broadcasted_iota(jnp.int32, (256, 32), 0) % 32
        == lax.broadcasted_iota(jnp.int32, (256, 32), 1)
    ).astype(F32).astype(BF16)
    widen = (
        lax.broadcasted_iota(jnp.int32, (32, 256), 1) // 8
        == lax.broadcasted_iota(jnp.int32, (32, 256), 0)
    ).astype(F32).astype(BF16)
    same = (
        lax.broadcasted_iota(jnp.int32, (256, 256), 0) // 32
        == lax.broadcasted_iota(jnp.int32, (256, 256), 1) % 8
    )
    small[0].wait()
    mix = [
        jnp.where(same, dot(dot(pick, part).astype(BF16), widen), 0.0).astype(BF16)
        for part in split2(root[...])
    ]

    small[1].wait()
    for b in range(6):
        latf[b * 128:(b + 1) * 128, :] = spread_rows(order[b:b + 1, :].astype(F32))
    lane = lax.broadcasted_iota(jnp.int32, (64, 128), 1)
    lane_f = lane.astype(F32)

    def choose(c):
        for q in range(4):
            rows = latf[pl.ds(c * 4 + q, 64, stride=12), :]
            for b in range(6):
                hit = rows == lane_f + float(b * 128)
                onehot[q * 64:(q + 1) * 64, b * 128:(b + 1) * 128] = jnp.where(
                    hit, 1.0, 0.0
                ).astype(BF16)

    choose(0)
    for k in range(4):
        pltpu.make_async_copy(control.at[k], ctrl.at[k], in_sem.at[k]).wait()
    small[2].wait()
    scale = loc[...]
    for r in range(2):
        for k in range(4):
            x = ctrl[k, :, r].reshape(256, 512)
            mixed = (dot(mix[0], x) + dot(mix[1], x)) * scale
            sp32[:, :, k] = mixed.reshape(8, 4, 8, 512)

        def narrow(s, _):
            spec[s, r * 128:(r + 1) * 128, :] = sp32[s].reshape(128, 512).astype(BF16)
            return 0

        lax.fori_loop(0, 8, narrow, 0)

    for s in range(8):
        pltpu.make_async_copy(legendre.at[s], leg.at[s], leg_sem.at[s]).wait()

    def transform(i, _):
        for d in range(4):
            s = i * 4 + d
            four[s] = dot(spec[s], leg[s]).astype(BF16)
        return 0

    lax.fori_loop(0, 2, transform, 0)

    pltpu.make_async_copy(perturb, pert, in_sem.at[4]).start()
    group = lane // 32
    me = mem * 64 + row
    pl.semaphore_wait(barrier, 255)

    def build(c, _):
        for s in range(8):
            picked = lax.dot_general(onehot[...], four[s], NT_DIMS, preferred_element_type=F32)
            for r in range(2):
                rolled = []
                for q in range(4):
                    part = picked[q * 64:(q + 1) * 64, r * 128:(r + 1) * 128]
                    rolled.append(pltpu.roll(part, q * 32, 1) if q else part)
                for level in range(4):
                    tile = rolled[(0 - level) % 4]
                    for g in range(1, 4):
                        tile = jnp.where(group == g, rolled[(g - level) % 4], tile)
                    msg[pl.ds(level * 16 + r * 8 + s, 64, stride=72), :] = tile

        def pack(b, _):
            for j in range(8):
                start = pl.multiple_of((b * 8 + j) * 72, 8)
                snd[c, pl.ds(b * 32 + j * 4, 4)] = (
                    msg[pl.ds(start, 64), :].reshape(4, 16, 128).astype(BF16)
                )
            return 0

        lax.fori_loop(0, 8, pack, 0)

        def send(r, m):
            pltpu.make_async_remote_copy(
                src_ref=snd.at[c, r * 4 + m],
                dst_ref=rcv.at[c, me],
                send_sem=send_sem.at[c],
                recv_sem=recv_sem.at[c, mem],
                device_id=(r, m),
                device_id_type=MESH,
            ).start()

        far_first(row, mem, send)
        rcv[c, me] = snd[c, row * 4 + mem]
        choose(lax.rem(c + 1, 3))
        return 0

    lax.fori_loop(0, 3, build, 0)

    small[3].wait()
    for b in range(4):
        wavef[b * 128:(b + 1) * 128, :] = spread_rows(waves[b:b + 1, :].astype(F32))

    def angles(wave, step):
        phase = wave * step
        phase = phase - 1536.0 * jnp.floor(phase * (1.0 / 1536.0))
        return phase * (2.0 * math.pi / 1536.0)

    def make_basis(b, _):
        wave = wavef[pl.ds(pl.multiple_of(b * 64, 64), 64), :]
        weight = jnp.where(wave == 0.0, 1.0, 2.0)
        near = angles(wave, lane_f)
        far = angles(wave, 128.0)
        cos, sin = weight * jnp.cos(near), weight * jnp.sin(near)
        turn_cos, turn_sin = jnp.cos(far), jnp.sin(far)
        for a in range(12):
            pair = jnp.stack([cos.reshape(8, 8, 128), -sin.reshape(8, 8, 128)], axis=1)
            basis[pl.ds(pl.multiple_of(b * 128, 128), 128), a * 128:(a + 1) * 128] = (
                pair.reshape(128, 128).astype(BF16)
            )
            cos, sin = cos * turn_cos - sin * turn_sin, sin * turn_cos + cos * turn_sin
        return 0

    lax.fori_loop(0, 8, make_basis, 0)
    pltpu.make_async_copy(perturb, pert, in_sem.at[4]).wait()

    def finish(c, _):
        for step, dx in enumerate((2, 1, 3, 0)):
            kg = lax.rem(mem + 4 - dx, 4)
            landed = rcv.at[c, pl.ds(0, 64 if dx else 63)]
            pltpu.make_async_copy(landed, landed, recv_sem.at[c, kg]).wait()
            lhs[...] = jnp.transpose(rcv[c, pl.ds(kg * 64, 64)].reshape(1024, 128))

            for n in range(6):
                cols = slice(n * 256, (n + 1) * 256)
                field = dot(lhs[...], basis[:, cols]).astype(BF16).astype(F32)
                field = field.reshape(4, 4, 8, 256)
                for g in range(4):
                    j = c * 4 + lax.rem(g + 4 - mem, 4)
                    weights = pert[j, pl.ds(kg * 4, 4), :, cols].astype(F32)
                    part = jnp.sum(field[g] * weights, axis=0)
                    if step:
                        part = part + total[g, :, cols]
                    if step == 3:
                        out[j, :, cols] = part.astype(BF16)
                    else:
                        total[g, :, cols] = part
        rows = pl.ds(c * 4, 4)
        pltpu.make_async_copy(out.at[rows], out_hbm.at[rows], out_sem.at[c]).start()
        pltpu.make_async_copy(
            snd.at[c, pl.ds(0, 255)], snd.at[c, pl.ds(0, 255)], send_sem.at[c]
        ).wait()
        return 0

    lax.fori_loop(0, 3, finish, 0)
    for c in range(3):
        rows = pl.ds(c * 4, 4)
        pltpu.make_async_copy(out.at[rows], out_hbm.at[rows], out_sem.at[c]).wait()


def shards(control, vert_root, loc_spec, legendre, wave_table, lat_order, perturb):
    hbm = pl.BlockSpec(memory_space=pl.ANY)
    return pl.pallas_call(
        kernel,
        name="synthesis",
        out_shape=jax.ShapeDtypeStruct((12, 8, 1536), BF16),
        in_specs=[hbm] * 7,
        out_specs=hbm,
        scratch_shapes=[
            pltpu.VMEM((32, 32), F32),
            pltpu.VMEM((1, 512), F32),
            pltpu.VMEM((4, 128), jnp.int32),
            pltpu.VMEM((6, 128), jnp.int32),
            pltpu.VMEM((12, 8, 1536), BF16),
            pltpu.VMEM((4, 32, 2, 8, 512), BF16),
            pltpu.VMEM((8, 512, 768), BF16),
            pltpu.VMEM((12, 16, 8, 1536), BF16),
            pltpu.VMEM((8, 4, 4, 8, 512), F32),
            pltpu.VMEM((8, 256, 512), BF16),
            pltpu.VMEM((8, 256, 768), BF16),
            pltpu.VMEM((768, 128), F32),
            pltpu.VMEM((256, 768), BF16),
            pltpu.VMEM((64 * 72, 128), F32),
            pltpu.VMEM((3, 256, 16, 128), BF16),
            pltpu.VMEM((3, 256, 16, 128), BF16),
            pltpu.VMEM((512, 128), F32),
            pltpu.VMEM((1024, 1536), BF16),
            pltpu.VMEM((128, 1024), BF16),
            pltpu.VMEM((4, 8, 1536), F32),
            pltpu.SemaphoreType.DMA((5,)),
            pltpu.SemaphoreType.DMA((8,)),
            pltpu.SemaphoreType.DMA((4,)),
            pltpu.SemaphoreType.DMA((3,)),
            pltpu.SemaphoreType.DMA((3,)),
            pltpu.SemaphoreType.DMA((3, 4)),
        ],
        compiler_params=pltpu.CompilerParams(
            collective_id=0, has_side_effects=True, vmem_limit_bytes=60 * 1024 * 1024
        ),
    )(
        control, vert_root, loc_spec.reshape(1, 512), legendre,
        wave_table.reshape(4, 128), lat_order.reshape(6, 128), perturb,
    )


def solution(mesh):
    return jax.shard_map(
        shards,
        mesh=mesh,
        in_specs=(
            P("mem", None, None, "rows", None),
            P(),
            P(),
            P("rows", None, None),
            P(),
            P(),
            P("rows", None, "mem", None),
        ),
        out_specs=P("rows", "mem", None),
        check_vma=False,
    )
```

```python
import functools
import math

import jax
import jax.numpy as jnp
from jax import lax
from jax.experimental import pallas as pl
from jax.experimental.pallas import tpu as pltpu
from jax.sharding import PartitionSpec as P

MESH = pl.DeviceIdType.MESH
F32, BF16 = jnp.float32, jnp.bfloat16
NT_DIMS = (((1,), (1,)), ((), ()))


def dot(a, b):
    return jnp.dot(a, b, preferred_element_type=F32)


def split2(a):
    hi = a.astype(BF16)
    return hi, (a - hi.astype(F32)).astype(BF16)


def spread_rows(row):
    return jnp.transpose(jnp.broadcast_to(row, (128, 128)))


def everyone_else(row, mem, act):
    mems = [mem] + [lax.rem(mem + d, 4) for d in range(1, 4)]
    for d in range(1, 4):
        act(row, mems[d])

    def whole_row(r, _):
        for m in mems:
            act(r, m)
        return 0

    lax.fori_loop(row + 1, 64, whole_row, 0)
    lax.fori_loop(0, row, whole_row, 0)


def far_first(row, mem, act):
    z, y, c = lax.div(row, 8), lax.rem(lax.div(row, 2), 4), lax.rem(row, 2)
    planes = [lax.rem(z + dz, 8) * 8 for dz in (4, 3, 5, 2, 6, 1, 7, 0)]
    cores = [1 - c, c]
    for dx in (2, 1, 3, 0):
        m = lax.rem(mem + dx, 4)

        def at(dy, skip, m=m):
            line = lax.rem(y + dy, 4) * 2
            for i, core in enumerate(cores):
                for j, plane in enumerate(planes):
                    if not (skip and i == 1 and j == 7):
                        act(plane + line + core, m)

        def step(t, _, at=at):
            at(3 - t, False)
            return 0

        lax.fori_loop(0, 4 if dx else 3, step, 0)
        if not dx:
            at(0, True)


def kernel(
    control, root_in, loc_in, legendre, waves_in, order_in, perturb, out_hbm,
    root, loc, waves, order, out,
    ctrl, leg, pert, sp32, spec, four, latf, mixing, onehot, msg, snd, rcv, wavef, basis, lhs, total,
    in_sem, leg_sem, small_sem, out_sem, send_sem, recv_sem,
):
    row, mem = lax.axis_index("rows"), lax.axis_index("mem")
    barrier = pltpu.get_barrier_semaphore()

    small = [
        pltpu.make_async_copy(src, dst, small_sem.at[i])
        for i, (src, dst) in enumerate(
            ((root_in, root), (order_in, order), (loc_in, loc), (waves_in, waves))
        )
    ]
    small[0].start()
    for k in range(4):
        pltpu.make_async_copy(control.at[k], ctrl.at[k], in_sem.at[k]).start()
    for copy in small[1:]:
        copy.start()

    def load_leg(half):
        for s in range(half * 4, half * 4 + 4):
            pltpu.make_async_copy(legendre.at[s], leg.at[s], leg_sem.at[s]).start()

    def greet(r, m):
        pl.semaphore_signal(barrier, inc=1, device_id=(r, m), device_id_type=MESH)

    load_leg(0)
    everyone_else(row, mem, greet)
    load_leg(1)

    pick = (
        lax.broadcasted_iota(jnp.int32, (256, 32), 0) % 32
        == lax.broadcasted_iota(jnp.int32, (256, 32), 1)
    ).astype(F32).astype(BF16)
    widen = (
        lax.broadcasted_iota(jnp.int32, (32, 256), 1) // 8
        == lax.broadcasted_iota(jnp.int32, (32, 256), 0)
    ).astype(F32).astype(BF16)
    same = (
        lax.broadcasted_iota(jnp.int32, (256, 256), 0) // 32
        == lax.broadcasted_iota(jnp.int32, (256, 256), 1) % 8
    )
    small[0].wait()
    mix = [
        jnp.where(same, dot(dot(pick, part).astype(BF16), widen), 0.0).astype(BF16)
        for part in split2(root[...])
    ]
    for half in range(2):
        for i, part in enumerate(mix):
            mixing[half, i * 128:(i + 1) * 128, :] = part[half * 128:(half + 1) * 128, :]

    small[1].wait()
    for b in range(6):
        latf[b * 128:(b + 1) * 128, :] = spread_rows(order[b:b + 1, :].astype(F32))
    lane = lax.broadcasted_iota(jnp.int32, (64, 128), 1)
    lane_f = lane.astype(F32)

    def choose(c):
        for q in range(4):
            rows = latf[pl.ds(c * 4 + q, 64, stride=12), :]
            for b in range(6):
                hit = rows == lane_f + float(b * 128)
                onehot[q * 64:(q + 1) * 64, b * 128:(b + 1) * 128] = jnp.where(
                    hit, 1.0, 0.0
                ).astype(BF16)

    choose(0)
    group = lane // 32
    me = mem * 64 + row

    def transform(half):
        for r in range(2):
            for k in range(4):
                if not half and not r:
                    pltpu.make_async_copy(control.at[k], ctrl.at[k], in_sem.at[k]).wait()
                both = dot(mixing[half], ctrl[k, :, r].reshape(256, 512))
                mixed = (both[:128] + both[128:]) * scale
                sp32[:, :, k] = mixed.reshape(4, 4, 8, 512)

            for s in range(4):
                spec[s, r * 128:(r + 1) * 128, :] = sp32[s].reshape(128, 512).astype(BF16)

        for s in range(half * 4, half * 4 + 4):
            pltpu.make_async_copy(legendre.at[s], leg.at[s], leg_sem.at[s]).wait()
        for s in range(4):
            four[half * 4 + s] = dot(spec[s], leg[half * 4 + s]).astype(BF16)

    def gather(half):
        for s in range(4):
            picked = lax.dot_general(
                onehot[...], four[half * 4 + s], NT_DIMS, preferred_element_type=F32
            )
            for r in range(2):
                rolled = []
                for q in range(4):
                    part = picked[q * 64:(q + 1) * 64, r * 128:(r + 1) * 128]
                    rolled.append(pltpu.roll(part, q * 32, 1) if q else part)
                for level in range(4):
                    tile = rolled[(0 - level) % 4]
                    for g in range(1, 4):
                        tile = jnp.where(group == g, rolled[(g - level) % 4], tile)
                    start = level * 16 + half * 8 + r * 4 + s
                    msg[pl.ds(start, 64, stride=72), :] = tile

    def send(src, dst, c, r, m):
        pltpu.make_async_remote_copy(
            src_ref=src,
            dst_ref=dst,
            send_sem=send_sem.at[c],
            recv_sem=recv_sem.at[c, mem],
            device_id=(r, m),
            device_id_type=MESH,
        ).start()

    small[2].wait()
    scale = loc[...]
    for half in range(2):
        transform(half)
        gather(half)

        def pack_half(b, _, half=half):
            for j in range(8):
                for level in range(4):
                    start = pl.multiple_of((b * 8 + j) * 72 + level * 16 + half * 8, 8)
                    snd[0, b * 32 + j * 4 + level, half] = msg[pl.ds(start, 8), :].astype(BF16)
            return 0

        lax.fori_loop(0, 8, pack_half, 0)
        if not half:
            pl.semaphore_wait(barrier, 255)

        def send_half(r, m, half=half):
            send(snd.at[0, r * 4 + m, half], rcv.at[0, me, half], 0, r, m)

        far_first(row, mem, send_half)
    pltpu.make_async_copy(perturb, pert, in_sem.at[4]).start()
    rcv[0, me] = snd[0, row * 4 + mem]

    def build(c, _):
        choose(c)
        for half in range(2):
            gather(half)

        def pack(b, _):
            for j in range(8):
                start = pl.multiple_of((b * 8 + j) * 72, 8)
                snd[c, pl.ds(b * 32 + j * 4, 4)] = (
                    msg[pl.ds(start, 64), :].reshape(4, 2, 8, 128).astype(BF16)
                )
            return 0

        lax.fori_loop(0, 8, pack, 0)

        def send_tile(r, m):
            send(snd.at[c, r * 4 + m], rcv.at[c, me], c, r, m)

        far_first(row, mem, send_tile)
        rcv[c, me] = snd[c, row * 4 + mem]
        return 0

    lax.fori_loop(1, 3, build, 0)

    small[3].wait()
    for b in range(4):
        latf[b * 128:(b + 1) * 128, :] = spread_rows(waves[b:b + 1, :].astype(F32))
    for s in range(4):
        wave = latf[pl.ds(s, 128, stride=4), :]
        for r in range(2):
            wavef[pl.ds(r * 4 + s, 128, stride=8), :] = wave
    turn = ((lax.broadcasted_iota(jnp.int32, (64, 128), 0) // 4) % 2).astype(F32) * 384.0

    def angles(phase):
        phase = phase - 1536.0 * jnp.floor(phase * (1.0 / 1536.0))
        return phase * (2.0 * math.pi / 1536.0)

    def make_basis(b, _):
        rows = pl.ds(pl.multiple_of(b * 64, 64), 64)
        wave = wavef[rows, :]
        weight = jnp.where(wave == 0.0, 1.0, 2.0)
        near = angles(wave * lane_f + turn)
        far = angles(wave * 128.0)
        cos, sin = weight * jnp.cos(near), weight * jnp.sin(near)
        turn_cos, turn_sin = jnp.cos(far), jnp.sin(far)
        for a in range(12):
            basis[rows, a * 128:(a + 1) * 128] = cos.astype(BF16)
            cos, sin = cos * turn_cos - sin * turn_sin, sin * turn_cos + cos * turn_sin
        return 0

    lax.fori_loop(0, 16, make_basis, 0)
    pltpu.make_async_copy(perturb, pert, in_sem.at[4]).wait()

    def finish(c, _):
        for step, dx in enumerate((2, 1, 3, 0)):
            kg = lax.rem(mem + 4 - dx, 4)
            landed = rcv.at[c, pl.ds(0, 64 if dx else 63)]
            pltpu.make_async_copy(landed, landed, recv_sem.at[c, kg]).wait()
            lhs[...] = jnp.transpose(rcv[c, pl.ds(kg * 64, 64)].reshape(1024, 128))

            for n in range(6):
                cols = slice(n * 256, (n + 1) * 256)
                field = dot(lhs[...], basis[:, cols]).astype(BF16).astype(F32)
                field = field.reshape(4, 4, 8, 256)
                for g in range(4):
                    j = c * 4 + lax.rem(g + 4 - mem, 4)
                    weights = pert[j, pl.ds(kg * 4, 4), :, cols].astype(F32)
                    part = jnp.sum(field[g] * weights, axis=0)
                    if step:
                        part = part + total[g, :, cols]
                    if step == 3:
                        out[j, :, cols] = part.astype(BF16)
                    else:
                        total[g, :, cols] = part
        rows = pl.ds(c * 4, 4)
        pltpu.make_async_copy(out.at[rows], out_hbm.at[rows], out_sem.at[c]).start()
        pltpu.make_async_copy(
            snd.at[c, pl.ds(0, 255)], snd.at[c, pl.ds(0, 255)], send_sem.at[c]
        ).wait()
        return 0

    lax.fori_loop(0, 3, finish, 0)
    for c in range(3):
        rows = pl.ds(c * 4, 4)
        pltpu.make_async_copy(out.at[rows], out_hbm.at[rows], out_sem.at[c]).wait()


def shards(control, vert_root, loc_spec, legendre, wave_table, lat_order, perturb):
    hbm = pl.BlockSpec(memory_space=pl.ANY)
    return pl.pallas_call(
        kernel,
        name="synthesis",
        out_shape=jax.ShapeDtypeStruct((12, 8, 1536), BF16),
        in_specs=[hbm] * 7,
        out_specs=hbm,
        scratch_shapes=[
            pltpu.VMEM((32, 32), F32),
            pltpu.VMEM((1, 512), F32),
            pltpu.VMEM((4, 128), jnp.int32),
            pltpu.VMEM((6, 128), jnp.int32),
            pltpu.VMEM((12, 8, 1536), BF16),
            pltpu.VMEM((4, 32, 2, 8, 512), BF16),
            pltpu.VMEM((8, 512, 768), BF16),
            pltpu.VMEM((12, 16, 8, 1536), BF16),
            pltpu.VMEM((4, 4, 4, 8, 512), F32),
            pltpu.VMEM((4, 256, 512), BF16),
            pltpu.VMEM((8, 256, 768), BF16),
            pltpu.VMEM((768, 128), F32),
            pltpu.VMEM((2, 256, 256), BF16),
            pltpu.VMEM((256, 768), BF16),
            pltpu.VMEM((64 * 72, 128), F32),
            pltpu.VMEM((3, 256, 2, 8, 128), BF16),
            pltpu.VMEM((3, 256, 2, 8, 128), BF16),
            pltpu.VMEM((1024, 128), F32),
            pltpu.VMEM((1024, 1536), BF16),
            pltpu.VMEM((128, 1024), BF16),
            pltpu.VMEM((4, 8, 1536), F32),
            pltpu.SemaphoreType.DMA((5,)),
            pltpu.SemaphoreType.DMA((8,)),
            pltpu.SemaphoreType.DMA((4,)),
            pltpu.SemaphoreType.DMA((3,)),
            pltpu.SemaphoreType.DMA((3,)),
            pltpu.SemaphoreType.DMA((3, 4)),
        ],
        compiler_params=pltpu.CompilerParams(
            collective_id=0, has_side_effects=True, vmem_limit_bytes=60 * 1024 * 1024
        ),
    )(
        control, vert_root, loc_spec.reshape(1, 512), legendre,
        wave_table.reshape(4, 128), lat_order.reshape(6, 128), perturb,
    )


def solution(mesh):
    return jax.shard_map(
        shards,
        mesh=mesh,
        in_specs=(
            P("mem", None, None, "rows", None),
            P(),
            P(),
            P("rows", None, None),
            P(),
            P(),
            P("rows", None, "mem", None),
        ),
        out_specs=P("rows", "mem", None),
        check_vma=False,
    )
```

```python
import functools
import math

import jax
import jax.numpy as jnp
from jax import lax
from jax.experimental import pallas as pl
from jax.experimental.pallas import tpu as pltpu
from jax.sharding import PartitionSpec as P

MESH = pl.DeviceIdType.MESH
F32, BF16 = jnp.float32, jnp.bfloat16
NT_DIMS = (((1,), (1,)), ((), ()))


def dot(a, b):
    return jnp.dot(a, b, preferred_element_type=F32)


def split2(a):
    hi = a.astype(BF16)
    return hi, (a - hi.astype(F32)).astype(BF16)


def spread_rows(row):
    return jnp.transpose(jnp.broadcast_to(row, (128, 128)))


def everyone_else(row, mem, act):
    mems = [mem] + [lax.rem(mem + d, 4) for d in range(1, 4)]
    for d in range(1, 4):
        act(row, mems[d])

    def whole_row(r, _):
        for m in mems:
            act(r, m)
        return 0

    lax.fori_loop(row + 1, 64, whole_row, 0)
    lax.fori_loop(0, row, whole_row, 0)


def far_first(row, mem, act):
    z, y, c = lax.div(row, 8), lax.rem(lax.div(row, 2), 4), lax.rem(row, 2)
    planes = [lax.rem(z + dz, 8) * 8 for dz in (4, 3, 5, 2, 6, 1, 7, 0)]
    cores = [1 - c, c]
    for dx in (2, 1, 3, 0):
        m = lax.rem(mem + dx, 4)

        def at(dy, skip, m=m):
            line = lax.rem(y + dy, 4) * 2
            for i, core in enumerate(cores):
                for j, plane in enumerate(planes):
                    if not (skip and i == 1 and j == 7):
                        act(plane + line + core, m)

        def step(t, _, at=at):
            at(3 - t, False)
            return 0

        lax.fori_loop(0, 4 if dx else 3, step, 0)
        if not dx:
            at(0, True)


def kernel(
    control, root_in, loc_in, legendre, waves_in, order_in, perturb, out,
    root, loc, waves, order,
    ctrl, leg, pert, sp32, spec, four, latf, mixing, onehot, msg, snd, rcv, wavef, basis, lhs, total,
    in_sem, leg_sem, small_sem, send_sem, recv_sem,
):
    row, mem = lax.axis_index("rows"), lax.axis_index("mem")
    barrier = pltpu.get_barrier_semaphore()

    small = [
        pltpu.make_async_copy(src, dst, small_sem.at[i])
        for i, (src, dst) in enumerate(
            ((root_in, root), (order_in, order), (loc_in, loc), (waves_in, waves))
        )
    ]
    small[0].start()
    for k in range(4):
        pltpu.make_async_copy(control.at[k], ctrl.at[k], in_sem.at[k]).start()
    for copy in small[1:]:
        copy.start()

    def load_leg(half):
        for s in range(half * 4, half * 4 + 4):
            pltpu.make_async_copy(legendre.at[s], leg.at[s], leg_sem.at[s]).start()

    def greet(r, m):
        pl.semaphore_signal(barrier, inc=1, device_id=(r, m), device_id_type=MESH)

    load_leg(0)
    everyone_else(row, mem, greet)
    load_leg(1)

    pick = (
        lax.broadcasted_iota(jnp.int32, (256, 32), 0) % 32
        == lax.broadcasted_iota(jnp.int32, (256, 32), 1)
    ).astype(F32).astype(BF16)
    widen = (
        lax.broadcasted_iota(jnp.int32, (32, 256), 1) // 8
        == lax.broadcasted_iota(jnp.int32, (32, 256), 0)
    ).astype(F32).astype(BF16)
    same = (
        lax.broadcasted_iota(jnp.int32, (256, 256), 0) // 32
        == lax.broadcasted_iota(jnp.int32, (256, 256), 1) % 8
    )
    small[0].wait()
    mix = [
        jnp.where(same, dot(dot(pick, part).astype(BF16), widen), 0.0).astype(BF16)
        for part in split2(root[...])
    ]
    for half in range(2):
        for i, part in enumerate(mix):
            mixing[half, i * 128:(i + 1) * 128, :] = part[half * 128:(half + 1) * 128, :]

    small[1].wait()
    for b in range(6):
        latf[b * 128:(b + 1) * 128, :] = spread_rows(order[b:b + 1, :].astype(F32))
    lane = lax.broadcasted_iota(jnp.int32, (64, 128), 1)
    lane_f = lane.astype(F32)

    def choose(c):
        for q in range(4):
            rows = latf[pl.ds(c * 4 + q, 64, stride=12), :]
            for b in range(6):
                hit = rows == lane_f + float(b * 128)
                onehot[q * 64:(q + 1) * 64, b * 128:(b + 1) * 128] = jnp.where(
                    hit, 1.0, 0.0
                ).astype(BF16)

    choose(0)
    group = lane // 32
    me = mem * 64 + row

    def transform(half):
        for r in range(2):
            for k in range(4):
                if not half and not r:
                    pltpu.make_async_copy(control.at[k], ctrl.at[k], in_sem.at[k]).wait()
                both = dot(mixing[half], ctrl[k, :, r].reshape(256, 512))
                mixed = (both[:128] + both[128:]) * scale
                sp32[:, :, k] = mixed.reshape(4, 4, 8, 512)

            for s in range(4):
                spec[s, r * 128:(r + 1) * 128, :] = sp32[s].reshape(128, 512).astype(BF16)

        for s in range(half * 4, half * 4 + 4):
            pltpu.make_async_copy(legendre.at[s], leg.at[s], leg_sem.at[s]).wait()
        for s in range(4):
            four[half * 4 + s] = dot(spec[s], leg[half * 4 + s]).astype(BF16)

    def gather(half):
        for s in range(4):
            picked = lax.dot_general(
                onehot[...], four[half * 4 + s], NT_DIMS, preferred_element_type=F32
            )
            for r in range(2):
                rolled = []
                for q in range(4):
                    part = picked[q * 64:(q + 1) * 64, r * 128:(r + 1) * 128]
                    rolled.append(pltpu.roll(part, q * 32, 1) if q else part)
                for level in range(4):
                    tile = rolled[(0 - level) % 4]
                    for g in range(1, 4):
                        tile = jnp.where(group == g, rolled[(g - level) % 4], tile)
                    start = level * 16 + half * 8 + r * 4 + s
                    msg[pl.ds(start, 64, stride=72), :] = tile

    def send(src, dst, c, r, m):
        pltpu.make_async_remote_copy(
            src_ref=src,
            dst_ref=dst,
            send_sem=send_sem.at[c],
            recv_sem=recv_sem.at[c, mem],
            device_id=(r, m),
            device_id_type=MESH,
        ).start()

    small[2].wait()
    scale = loc[...]
    for half in range(2):
        transform(half)
        gather(half)

        def pack_half(b, _, half=half):
            for j in range(8):
                for level in range(4):
                    start = pl.multiple_of((b * 8 + j) * 72 + level * 16 + half * 8, 8)
                    snd[0, b * 32 + j * 4 + level, half] = msg[pl.ds(start, 8), :].astype(BF16)
            return 0

        lax.fori_loop(0, 8, pack_half, 0)
        if not half:
            pl.semaphore_wait(barrier, 255)

        def send_half(r, m, half=half):
            send(snd.at[0, r * 4 + m, half], rcv.at[0, me, half], 0, r, m)

        far_first(row, mem, send_half)
    pltpu.make_async_copy(perturb, pert, in_sem.at[4]).start()
    rcv[0, me] = snd[0, row * 4 + mem]

    def build(c, _):
        choose(c)
        for half in range(2):
            gather(half)

        def pack(b, _):
            for j in range(8):
                start = pl.multiple_of((b * 8 + j) * 72, 8)
                snd[c, pl.ds(b * 32 + j * 4, 4)] = (
                    msg[pl.ds(start, 64), :].reshape(4, 2, 8, 128).astype(BF16)
                )
            return 0

        lax.fori_loop(0, 8, pack, 0)

        def send_tile(r, m):
            send(snd.at[c, r * 4 + m], rcv.at[c, me], c, r, m)

        far_first(row, mem, send_tile)
        rcv[c, me] = snd[c, row * 4 + mem]
        return 0

    lax.fori_loop(1, 3, build, 0)

    small[3].wait()
    for b in range(4):
        latf[b * 128:(b + 1) * 128, :] = spread_rows(waves[b:b + 1, :].astype(F32))
    for s in range(4):
        wave = latf[pl.ds(s, 128, stride=4), :]
        for r in range(2):
            wavef[pl.ds(r * 4 + s, 128, stride=8), :] = wave
    turn = ((lax.broadcasted_iota(jnp.int32, (64, 128), 0) // 4) % 2).astype(F32) * 384.0

    def angles(phase):
        phase = phase - 1536.0 * jnp.floor(phase * (1.0 / 1536.0))
        return phase * (2.0 * math.pi / 1536.0)

    def make_basis(b, _):
        rows = pl.ds(pl.multiple_of(b * 64, 64), 64)
        wave = wavef[rows, :]
        weight = jnp.where(wave == 0.0, 1.0, 2.0)
        near = angles(wave * lane_f + turn)
        far = angles(wave * 128.0)
        cos, sin = weight * jnp.cos(near), weight * jnp.sin(near)
        turn_cos, turn_sin = jnp.cos(far), jnp.sin(far)
        for a in range(12):
            basis[rows, a * 128:(a + 1) * 128] = cos.astype(BF16)
            cos, sin = cos * turn_cos - sin * turn_sin, sin * turn_cos + cos * turn_sin
        return 0

    lax.fori_loop(0, 16, make_basis, 0)
    pltpu.make_async_copy(perturb, pert, in_sem.at[4]).wait()

    def finish(c, _):
        for step, dx in enumerate((2, 1, 3, 0)):
            kg = lax.rem(mem + 4 - dx, 4)
            landed = rcv.at[c, pl.ds(0, 64 if dx else 63)]
            pltpu.make_async_copy(landed, landed, recv_sem.at[c, kg]).wait()
            lhs[...] = jnp.transpose(rcv[c, pl.ds(kg * 64, 64)].reshape(1024, 128))

            for n in range(6):
                cols = slice(n * 256, (n + 1) * 256)
                field = dot(lhs[...], basis[:, cols]).astype(BF16).astype(F32)
                field = field.reshape(4, 4, 8, 256)
                for g in range(4):
                    j = c * 4 + lax.rem(g + 4 - mem, 4)
                    weights = pert[j, pl.ds(kg * 4, 4), :, cols].astype(F32)
                    part = jnp.sum(field[g] * weights, axis=0)
                    if step:
                        part = part + total[g, :, cols]
                    if step == 3:
                        out[j, :, cols] = part.astype(BF16)
                    else:
                        total[g, :, cols] = part
        pltpu.make_async_copy(
            snd.at[c, pl.ds(0, 255)], snd.at[c, pl.ds(0, 255)], send_sem.at[c]
        ).wait()
        return 0

    lax.fori_loop(0, 3, finish, 0)


def shards(control, vert_root, loc_spec, legendre, wave_table, lat_order, perturb):
    hbm = pl.BlockSpec(memory_space=pl.ANY)
    return pl.pallas_call(
        kernel,
        name="synthesis",
        out_shape=pltpu.VMEM((12, 8, 1536), BF16),
        in_specs=[hbm] * 7,
        out_specs=pl.BlockSpec(memory_space=pltpu.VMEM),
        scratch_shapes=[
            pltpu.VMEM((32, 32), F32),
            pltpu.VMEM((1, 512), F32),
            pltpu.VMEM((4, 128), jnp.int32),
            pltpu.VMEM((6, 128), jnp.int32),
            pltpu.VMEM((4, 32, 2, 8, 512), BF16),
            pltpu.VMEM((8, 512, 768), BF16),
            pltpu.VMEM((12, 16, 8, 1536), BF16),
            pltpu.VMEM((4, 4, 4, 8, 512), F32),
            pltpu.VMEM((4, 256, 512), BF16),
            pltpu.VMEM((8, 256, 768), BF16),
            pltpu.VMEM((768, 128), F32),
            pltpu.VMEM((2, 256, 256), BF16),
            pltpu.VMEM((256, 768), BF16),
            pltpu.VMEM((64 * 72, 128), F32),
            pltpu.VMEM((3, 256, 2, 8, 128), BF16),
            pltpu.VMEM((3, 256, 2, 8, 128), BF16),
            pltpu.VMEM((1024, 128), F32),
            pltpu.VMEM((1024, 1536), BF16),
            pltpu.VMEM((128, 1024), BF16),
            pltpu.VMEM((4, 8, 1536), F32),
            pltpu.SemaphoreType.DMA((5,)),
            pltpu.SemaphoreType.DMA((8,)),
            pltpu.SemaphoreType.DMA((4,)),
            pltpu.SemaphoreType.DMA((3,)),
            pltpu.SemaphoreType.DMA((3, 4)),
        ],
        compiler_params=pltpu.CompilerParams(
            collective_id=0, has_side_effects=True, vmem_limit_bytes=60 * 1024 * 1024
        ),
    )(
        control, vert_root, loc_spec.reshape(1, 512), legendre,
        wave_table.reshape(4, 128), lat_order.reshape(6, 128), perturb,
    )


def solution(mesh):
    return jax.shard_map(
        shards,
        mesh=mesh,
        in_specs=(
            P("mem", None, None, "rows", None),
            P(),
            P(),
            P("rows", None, None),
            P(),
            P(),
            P("rows", None, "mem", None),
        ),
        out_specs=P("rows", "mem", None),
        check_vma=False,
    )
```

```python
import functools
import math

import jax
import jax.numpy as jnp
from jax import lax
from jax.experimental import pallas as pl
from jax.experimental.pallas import tpu as pltpu
from jax.sharding import PartitionSpec as P

MESH = pl.DeviceIdType.MESH
F32, BF16 = jnp.float32, jnp.bfloat16
NT_DIMS = (((1,), (1,)), ((), ()))


def dot(a, b):
    return jnp.dot(a, b, preferred_element_type=F32)


def split2(a):
    hi = a.astype(BF16)
    return hi, (a - hi.astype(F32)).astype(BF16)


def spread_rows(row):
    return jnp.transpose(jnp.broadcast_to(row, (128, 128)))


def everyone_else(row, mem, act, between):
    mems = [mem] + [lax.rem(mem + d, 4) for d in range(1, 4)]
    for d in range(1, 4):
        act(row, mems[d])

    def whole_row(r, _):
        for m in mems:
            act(r, m)
        return 0

    lax.fori_loop(row + 1, 64, whole_row, 0)
    between()
    lax.fori_loop(0, row, whole_row, 0)


def far_first(row, mem, act):
    z, y, c = lax.div(row, 8), lax.rem(lax.div(row, 2), 4), lax.rem(row, 2)
    planes = [lax.rem(z + dz, 8) * 8 for dz in (4, 3, 5, 2, 6, 1, 7, 0)]
    cores = [1 - c, c]
    for dx in (2, 1, 3, 0):
        m = lax.rem(mem + dx, 4)

        def at(dy, skip, m=m):
            line = lax.rem(y + dy, 4) * 2
            for i, core in enumerate(cores):
                for j, plane in enumerate(planes):
                    if not (skip and i == 1 and j == 7):
                        act(plane + line + core, m)

        def step(t, _, at=at):
            at(3 - t, False)
            return 0

        lax.fori_loop(0, 4 if dx else 3, step, 0)
        if not dx:
            at(0, True)


def far_first_mixed(row, mem, act):
    z, y, c = lax.div(row, 8), lax.rem(lax.div(row, 2), 4), lax.rem(row, 2)
    planes = [lax.rem(z + dz, 8) * 8 for dz in (4, 3, 5, 2, 6, 1, 7, 0)]
    mems = [lax.rem(mem + dx, 4) for dx in (2, 1, 3)] + [mem]

    def at(dy, core, skip):
        line = lax.rem(y + dy, 4) * 2 + core
        for j, plane in enumerate(planes):
            for i, m in enumerate(mems):
                if not (skip and j == 7 and i == 3):
                    act(plane + line, m)

    def step(t, _):
        dy = 3 - lax.div(t, 2)
        at(dy, lax.rem(c + 1 + t, 2), False)
        return 0

    lax.fori_loop(0, 7, step, 0)
    at(0, c, True)


def kernel(
    control, root_in, loc_in, legendre, waves_in, order_in, perturb, out,
    root, loc, waves, order,
    ctrl, leg, pert, sp32, spec, four, latf, mixing, onehot, msg, snd, rcv, wavef, basis, lhs, total,
    in_sem, leg_sem, small_sem, send_sem, recv_sem,
):
    row, mem = lax.axis_index("rows"), lax.axis_index("mem")
    barrier = pltpu.get_barrier_semaphore()

    small = [
        pltpu.make_async_copy(src, dst, small_sem.at[i])
        for i, (src, dst) in enumerate(
            ((root_in, root), (order_in, order), (loc_in, loc), (waves_in, waves))
        )
    ]
    small[0].start()
    for k in range(4):
        pltpu.make_async_copy(control.at[k], ctrl.at[k], in_sem.at[k]).start()
    for copy in small[1:]:
        copy.start()

    def load_leg(half):
        for s in range(half * 4, half * 4 + 4):
            pltpu.make_async_copy(legendre.at[s], leg.at[s], leg_sem.at[s]).start()

    def greet(r, m):
        pl.semaphore_signal(barrier, inc=1, device_id=(r, m), device_id_type=MESH)

    everyone_else(row, mem, greet, lambda: load_leg(0))
    load_leg(1)

    pick = (
        lax.broadcasted_iota(jnp.int32, (256, 32), 0) % 32
        == lax.broadcasted_iota(jnp.int32, (256, 32), 1)
    ).astype(F32).astype(BF16)
    widen = (
        lax.broadcasted_iota(jnp.int32, (32, 256), 1) // 8
        == lax.broadcasted_iota(jnp.int32, (32, 256), 0)
    ).astype(F32).astype(BF16)
    same = (
        lax.broadcasted_iota(jnp.int32, (256, 256), 0) // 32
        == lax.broadcasted_iota(jnp.int32, (256, 256), 1) % 8
    )
    small[0].wait()
    mix = [
        jnp.where(same, dot(dot(pick, part).astype(BF16), widen), 0.0).astype(BF16)
        for part in split2(root[...])
    ]
    for half in range(2):
        for i, part in enumerate(mix):
            mixing[half, i * 128:(i + 1) * 128, :] = part[half * 128:(half + 1) * 128, :]

    small[1].wait()
    for b in range(6):
        latf[b * 128:(b + 1) * 128, :] = spread_rows(order[b:b + 1, :].astype(F32))
    lane = lax.broadcasted_iota(jnp.int32, (64, 128), 1)
    lane_f = lane.astype(F32)

    def choose(c):
        for q in range(4):
            rows = latf[pl.ds(c * 4 + q, 64, stride=12), :]
            for b in range(6):
                hit = rows == lane_f + float(b * 128)
                onehot[q * 64:(q + 1) * 64, b * 128:(b + 1) * 128] = jnp.where(
                    hit, 1.0, 0.0
                ).astype(BF16)

    choose(0)
    group = lane // 32
    me = mem * 64 + row

    def transform(half):
        for r in range(2):
            for k in range(4):
                both = dot(mixing[half], ctrl[k, :, r].reshape(256, 512))
                mixed = (both[:128] + both[128:]) * scale
                sp32[:, :, k] = mixed.reshape(4, 4, 8, 512)

            for s in range(4):
                spec[s, r * 128:(r + 1) * 128, :] = sp32[s].reshape(128, 512).astype(BF16)

        for s in range(half * 4, half * 4 + 4):
            pltpu.make_async_copy(legendre.at[s], leg.at[s], leg_sem.at[s]).wait()
        for s in range(4):
            four[half * 4 + s] = dot(spec[s], leg[half * 4 + s]).astype(BF16)

    def gather(half):
        for s in range(4):
            picked = lax.dot_general(
                onehot[...], four[half * 4 + s], NT_DIMS, preferred_element_type=F32
            )
            for r in range(2):
                rolled = []
                for q in range(4):
                    part = picked[q * 64:(q + 1) * 64, r * 128:(r + 1) * 128]
                    rolled.append(pltpu.roll(part, q * 32, 1) if q else part)
                for level in range(4):
                    tile = rolled[(0 - level) % 4]
                    for g in range(1, 4):
                        tile = jnp.where(group == g, rolled[(g - level) % 4], tile)
                    start = level * 16 + half * 8 + r * 4 + s
                    msg[pl.ds(start, 64, stride=72), :] = tile

    def send(src, dst, c, r, m):
        pltpu.make_async_remote_copy(
            src_ref=src,
            dst_ref=dst,
            send_sem=send_sem.at[c],
            recv_sem=recv_sem.at[c, mem],
            device_id=(r, m),
            device_id_type=MESH,
        ).start()

    small[2].wait()
    scale = loc[...]
    for k in range(4):
        pltpu.make_async_copy(control.at[k], ctrl.at[k], in_sem.at[k]).wait()
    for half in range(2):
        transform(half)
        gather(half)

        def pack_half(b, _, half=half):
            for j in range(8):
                for level in range(4):
                    start = pl.multiple_of((b * 8 + j) * 72 + level * 16 + half * 8, 8)
                    snd[0, b * 32 + j * 4 + level, half] = msg[pl.ds(start, 8), :].astype(BF16)
            return 0

        lax.fori_loop(0, 8, pack_half, 0)
        if not half:
            pl.semaphore_wait(barrier, 255)

        def send_half(r, m, half=half):
            send(snd.at[0, r * 4 + m, half], rcv.at[0, me, half], 0, r, m)

        far_first_mixed(row, mem, send_half)
    pltpu.make_async_copy(perturb, pert, in_sem.at[4]).start()
    rcv[0, me] = snd[0, row * 4 + mem]

    def build(c, _):
        choose(c)
        for half in range(2):
            gather(half)

        def pack(b, _):
            for j in range(8):
                start = pl.multiple_of((b * 8 + j) * 72, 8)
                snd[c, pl.ds(b * 32 + j * 4, 4)] = (
                    msg[pl.ds(start, 64), :].reshape(4, 2, 8, 128).astype(BF16)
                )
            return 0

        lax.fori_loop(0, 8, pack, 0)

        def send_tile(r, m):
            send(snd.at[c, r * 4 + m], rcv.at[c, me], c, r, m)

        far_first(row, mem, send_tile)
        rcv[c, me] = snd[c, row * 4 + mem]
        return 0

    lax.fori_loop(1, 3, build, 0)

    small[3].wait()
    for b in range(4):
        latf[b * 128:(b + 1) * 128, :] = spread_rows(waves[b:b + 1, :].astype(F32))
    for s in range(4):
        wave = latf[pl.ds(s, 128, stride=4), :]
        for r in range(2):
            wavef[pl.ds(r * 4 + s, 128, stride=8), :] = wave
    turn = ((lax.broadcasted_iota(jnp.int32, (64, 128), 0) // 4) % 2).astype(F32) * 384.0

    def angles(phase):
        phase = phase - 1536.0 * jnp.floor(phase * (1.0 / 1536.0))
        return phase * (2.0 * math.pi / 1536.0)

    def make_basis(b, _):
        rows = pl.ds(pl.multiple_of(b * 64, 64), 64)
        wave = wavef[rows, :]
        weight = jnp.where(wave == 0.0, 1.0, 2.0)
        near = angles(wave * lane_f + turn)
        far = angles(wave * 128.0)
        cos, sin = weight * jnp.cos(near), weight * jnp.sin(near)
        turn_cos, turn_sin = jnp.cos(far), jnp.sin(far)
        for a in range(12):
            basis[rows, a * 128:(a + 1) * 128] = cos.astype(BF16)
            cos, sin = cos * turn_cos - sin * turn_sin, sin * turn_cos + cos * turn_sin
        return 0

    lax.fori_loop(0, 16, make_basis, 0)
    pltpu.make_async_copy(perturb, pert, in_sem.at[4]).wait()

    def finish(c, _):
        for step, dx in enumerate((2, 1, 3, 0)):
            kg = lax.rem(mem + 4 - dx, 4)
            landed = rcv.at[c, pl.ds(0, 64 if dx else 63)]
            pltpu.make_async_copy(landed, landed, recv_sem.at[c, kg]).wait()
            lhs[...] = jnp.transpose(rcv[c, pl.ds(kg * 64, 64)].reshape(1024, 128))

            for n in range(6):
                cols = slice(n * 256, (n + 1) * 256)
                field = dot(lhs[...], basis[:, cols]).astype(BF16).astype(F32)
                field = field.reshape(4, 4, 8, 256)
                for g in range(4):
                    j = c * 4 + lax.rem(g + 4 - mem, 4)
                    weights = pert[j, pl.ds(kg * 4, 4), :, cols].astype(F32)
                    part = jnp.sum(field[g] * weights, axis=0)
                    if step:
                        part = part + total[g, :, cols]
                    if step == 3:
                        out[j, :, cols] = part.astype(BF16)
                    else:
                        total[g, :, cols] = part
        pltpu.make_async_copy(
            snd.at[c, pl.ds(0, 255)], snd.at[c, pl.ds(0, 255)], send_sem.at[c]
        ).wait()
        return 0

    lax.fori_loop(0, 3, finish, 0)


def shards(control, vert_root, loc_spec, legendre, wave_table, lat_order, perturb):
    hbm = pl.BlockSpec(memory_space=pl.ANY)
    return pl.pallas_call(
        kernel,
        name="synthesis",
        out_shape=pltpu.VMEM((12, 8, 1536), BF16),
        in_specs=[hbm] * 7,
        out_specs=pl.BlockSpec(memory_space=pltpu.VMEM),
        scratch_shapes=[
            pltpu.VMEM((32, 32), F32),
            pltpu.VMEM((1, 512), F32),
            pltpu.VMEM((4, 128), jnp.int32),
            pltpu.VMEM((6, 128), jnp.int32),
            pltpu.VMEM((4, 32, 2, 8, 512), BF16),
            pltpu.VMEM((8, 512, 768), BF16),
            pltpu.VMEM((12, 16, 8, 1536), BF16),
            pltpu.VMEM((4, 4, 4, 8, 512), F32),
            pltpu.VMEM((4, 256, 512), BF16),
            pltpu.VMEM((8, 256, 768), BF16),
            pltpu.VMEM((768, 128), F32),
            pltpu.VMEM((2, 256, 256), BF16),
            pltpu.VMEM((256, 768), BF16),
            pltpu.VMEM((64 * 72, 128), F32),
            pltpu.VMEM((3, 256, 2, 8, 128), BF16),
            pltpu.VMEM((3, 256, 2, 8, 128), BF16),
            pltpu.VMEM((1024, 128), F32),
            pltpu.VMEM((1024, 1536), BF16),
            pltpu.VMEM((128, 1024), BF16),
            pltpu.VMEM((4, 8, 1536), F32),
            pltpu.SemaphoreType.DMA((5,)),
            pltpu.SemaphoreType.DMA((8,)),
            pltpu.SemaphoreType.DMA((4,)),
            pltpu.SemaphoreType.DMA((3,)),
            pltpu.SemaphoreType.DMA((3, 4)),
        ],
        compiler_params=pltpu.CompilerParams(
            collective_id=0, has_side_effects=True, vmem_limit_bytes=60 * 1024 * 1024
        ),
    )(
        control, vert_root, loc_spec.reshape(1, 512), legendre,
        wave_table.reshape(4, 128), lat_order.reshape(6, 128), perturb,
    )


def solution(mesh):
    return jax.shard_map(
        shards,
        mesh=mesh,
        in_specs=(
            P("mem", None, None, "rows", None),
            P(),
            P(),
            P("rows", None, None),
            P(),
            P(),
            P("rows", None, "mem", None),
        ),
        out_specs=P("rows", "mem", None),
        check_vma=False,
    )
```

```python
import functools
import math

import jax
import jax.numpy as jnp
from jax import lax
from jax.experimental import pallas as pl
from jax.experimental.pallas import tpu as pltpu
from jax.sharding import PartitionSpec as P

MESH = pl.DeviceIdType.MESH
F32, BF16 = jnp.float32, jnp.bfloat16
NT_DIMS = (((1,), (1,)), ((), ()))


def dot(a, b):
    return jnp.dot(a, b, preferred_element_type=F32)


def split2(a):
    hi = a.astype(BF16)
    return hi, (a - hi.astype(F32)).astype(BF16)


def spread_rows(row):
    return jnp.transpose(jnp.broadcast_to(row, (128, 128)))


def everyone_else(row, mem, act, between):
    mems = [mem] + [lax.rem(mem + d, 4) for d in range(1, 4)]
    for d in range(1, 4):
        act(row, mems[d])

    def whole_row(r, _):
        for m in mems:
            act(r, m)
        return 0

    lax.fori_loop(row + 1, 64, whole_row, 0)
    between()
    lax.fori_loop(0, row, whole_row, 0)


def far_first(row, mem, act):
    z, y, c = lax.div(row, 8), lax.rem(lax.div(row, 2), 4), lax.rem(row, 2)
    planes = [lax.rem(z + dz, 8) * 8 for dz in (4, 3, 5, 2, 6, 1, 7, 0)]
    cores = [1 - c, c]
    for dx in (2, 1, 3, 0):
        m = lax.rem(mem + dx, 4)

        def at(dy, skip, m=m):
            line = lax.rem(y + dy, 4) * 2
            for i, core in enumerate(cores):
                for j, plane in enumerate(planes):
                    if not (skip and i == 1 and j == 7):
                        act(plane + line + core, m)

        def step(t, _, at=at):
            at(3 - t, False)
            return 0

        lax.fori_loop(0, 4 if dx else 3, step, 0)
        if not dx:
            at(0, True)


def far_first_mixed(row, mem, act):
    z, y, c = lax.div(row, 8), lax.rem(lax.div(row, 2), 4), lax.rem(row, 2)
    planes = [lax.rem(z + dz, 8) * 8 for dz in (4, 3, 5, 2, 6, 1, 7, 0)]
    mems = [lax.rem(mem + dx, 4) for dx in (2, 1, 3)] + [mem]

    def at(dy, core, skip):
        line = lax.rem(y + dy, 4) * 2 + core
        for j, plane in enumerate(planes):
            for i, m in enumerate(mems):
                if not (skip and j == 7 and i == 3):
                    act(plane + line, m)

    def step(t, _):
        dy = 3 - lax.div(t, 2)
        at(dy, lax.rem(c + 1 + t, 2), False)
        return 0

    lax.fori_loop(0, 7, step, 0)
    at(0, c, True)


def kernel(
    control, root_in, loc_in, legendre, waves_in, order_in, perturb, out,
    root, loc, waves, order,
    ctrl, leg, pert, sp32, spec, four, latf, mixing, onehot, msg, snd, rcv, wavef, basis, lhs, total,
    in_sem, leg_sem, small_sem, send_sem, recv_sem,
):
    row, mem = lax.axis_index("rows"), lax.axis_index("mem")
    barrier = pltpu.get_barrier_semaphore()

    small = [
        pltpu.make_async_copy(src, dst, small_sem.at[i])
        for i, (src, dst) in enumerate(
            ((root_in, root), (order_in, order), (loc_in, loc), (waves_in, waves))
        )
    ]
    small[0].start()
    for k in range(4):
        pltpu.make_async_copy(control.at[k], ctrl.at[k], in_sem.at[k]).start()
    for copy in small[1:]:
        copy.start()

    def load_leg(half):
        for s in range(half * 4, half * 4 + 4):
            pltpu.make_async_copy(legendre.at[s], leg.at[s], leg_sem.at[s]).start()

    def greet(r, m):
        pl.semaphore_signal(barrier, inc=1, device_id=(r, m), device_id_type=MESH)

    everyone_else(row, mem, greet, lambda: load_leg(0))
    load_leg(1)

    pick = (
        lax.broadcasted_iota(jnp.int32, (256, 32), 0) % 32
        == lax.broadcasted_iota(jnp.int32, (256, 32), 1)
    ).astype(F32).astype(BF16)
    widen = (
        lax.broadcasted_iota(jnp.int32, (32, 256), 1) // 8
        == lax.broadcasted_iota(jnp.int32, (32, 256), 0)
    ).astype(F32).astype(BF16)
    same = (
        lax.broadcasted_iota(jnp.int32, (256, 256), 0) // 32
        == lax.broadcasted_iota(jnp.int32, (256, 256), 1) % 8
    )
    small[0].wait()
    mix = [
        jnp.where(same, dot(dot(pick, part).astype(BF16), widen), 0.0).astype(BF16)
        for part in split2(root[...])
    ]
    for half in range(2):
        for i, part in enumerate(mix):
            mixing[half, i * 128:(i + 1) * 128, :] = part[half * 128:(half + 1) * 128, :]

    small[1].wait()
    for b in range(6):
        latf[b * 128:(b + 1) * 128, :] = spread_rows(order[b:b + 1, :].astype(F32))
    lane = lax.broadcasted_iota(jnp.int32, (64, 128), 1)
    lane_f = lane.astype(F32)

    def choose(c):
        for q in range(4):
            rows = latf[pl.ds(c * 4 + q, 64, stride=12), :]
            for b in range(6):
                hit = rows == lane_f + float(b * 128)
                onehot[q * 64:(q + 1) * 64, b * 128:(b + 1) * 128] = jnp.where(
                    hit, 1.0, 0.0
                ).astype(BF16)

    choose(0)
    group = lane // 32
    me = mem * 64 + row

    def transform(half):
        for r in range(2):
            for k in range(4):
                both = dot(mixing[half], ctrl[k, :, r].reshape(256, 512))
                mixed = (both[:128] + both[128:]) * scale
                sp32[:, :, k] = mixed.reshape(4, 4, 8, 512)

            for s in range(4):
                spec[s, r * 128:(r + 1) * 128, :] = sp32[s].reshape(128, 512).astype(BF16)

        for s in range(half * 4, half * 4 + 4):
            pltpu.make_async_copy(legendre.at[s], leg.at[s], leg_sem.at[s]).wait()
        for s in range(4):
            four[half * 4 + s] = dot(spec[s], leg[half * 4 + s]).astype(BF16)

    def gather(half):
        for s in range(4):
            picked = lax.dot_general(
                onehot[...], four[half * 4 + s], NT_DIMS, preferred_element_type=F32
            )
            for r in range(2):
                rolled = []
                for q in range(4):
                    part = picked[q * 64:(q + 1) * 64, r * 128:(r + 1) * 128]
                    rolled.append(pltpu.roll(part, q * 32, 1) if q else part)
                for level in range(4):
                    tile = rolled[(0 - level) % 4]
                    for g in range(1, 4):
                        tile = jnp.where(group == g, rolled[(g - level) % 4], tile)
                    start = level * 16 + half * 8 + r * 4 + s
                    msg[pl.ds(start, 64, stride=72), :] = tile

    def send(src, dst, c, r, m):
        pltpu.make_async_remote_copy(
            src_ref=src,
            dst_ref=dst,
            send_sem=send_sem.at[c],
            recv_sem=recv_sem.at[c, mem],
            device_id=(r, m),
            device_id_type=MESH,
        ).start()

    small[2].wait()
    scale = loc[...]
    for k in range(4):
        pltpu.make_async_copy(control.at[k], ctrl.at[k], in_sem.at[k]).wait()
    for half in range(2):
        transform(half)
        gather(half)

        def pack_half(b, _, half=half):
            for j in range(8):
                for level in range(4):
                    start = pl.multiple_of((b * 8 + j) * 72 + level * 16 + half * 8, 8)
                    snd[0, b * 32 + j * 4 + level, half] = msg[pl.ds(start, 8), :].astype(BF16)
            return 0

        lax.fori_loop(0, 8, pack_half, 0)
        if not half:
            pl.semaphore_wait(barrier, 255)

        def send_half(r, m, half=half):
            send(snd.at[0, r * 4 + m, half], rcv.at[0, me, half], 0, r, m)

        far_first_mixed(row, mem, send_half)
    pltpu.make_async_copy(perturb, pert, in_sem.at[4]).start()
    rcv[0, me] = snd[0, row * 4 + mem]

    def build(c):
        choose(c)
        for half in range(2):
            gather(half)

        def pack(b, _):
            for j in range(8):
                start = pl.multiple_of((b * 8 + j) * 72, 8)
                snd[c, pl.ds(b * 32 + j * 4, 4)] = (
                    msg[pl.ds(start, 64), :].reshape(4, 2, 8, 128).astype(BF16)
                )
            return 0

        lax.fori_loop(0, 8, pack, 0)

        def send_tile(r, m):
            send(snd.at[c, r * 4 + m], rcv.at[c, me], c, r, m)

        (far_first_mixed if c == 1 else far_first)(row, mem, send_tile)
        rcv[c, me] = snd[c, row * 4 + mem]

    for c in (1, 2):
        build(c)

    small[3].wait()
    for b in range(4):
        latf[b * 128:(b + 1) * 128, :] = spread_rows(waves[b:b + 1, :].astype(F32))
    for s in range(4):
        wave = latf[pl.ds(s, 128, stride=4), :]
        for r in range(2):
            wavef[pl.ds(r * 4 + s, 128, stride=8), :] = wave
    turn = ((lax.broadcasted_iota(jnp.int32, (64, 128), 0) // 4) % 2).astype(F32) * 384.0

    def angles(phase):
        phase = phase - 1536.0 * jnp.floor(phase * (1.0 / 1536.0))
        return phase * (2.0 * math.pi / 1536.0)

    def make_basis(b, _):
        rows = pl.ds(pl.multiple_of(b * 64, 64), 64)
        wave = wavef[rows, :]
        weight = jnp.where(wave == 0.0, 1.0, 2.0)
        near = angles(wave * lane_f + turn)
        far = angles(wave * 128.0)
        cos, sin = weight * jnp.cos(near), weight * jnp.sin(near)
        turn_cos, turn_sin = jnp.cos(far), jnp.sin(far)
        for a in range(12):
            basis[rows, a * 128:(a + 1) * 128] = cos.astype(BF16)
            cos, sin = cos * turn_cos - sin * turn_sin, sin * turn_cos + cos * turn_sin
        return 0

    lax.fori_loop(0, 16, make_basis, 0)
    pltpu.make_async_copy(perturb, pert, in_sem.at[4]).wait()

    def finish(c, _):
        for step, dx in enumerate((2, 1, 3, 0)):
            kg = lax.rem(mem + 4 - dx, 4)
            landed = rcv.at[c, pl.ds(0, 64 if dx else 63)]
            pltpu.make_async_copy(landed, landed, recv_sem.at[c, kg]).wait()
            lhs[...] = jnp.transpose(rcv[c, pl.ds(kg * 64, 64)].reshape(1024, 128))

            for n in range(6):
                cols = slice(n * 256, (n + 1) * 256)
                field = dot(lhs[...], basis[:, cols]).astype(BF16).astype(F32)
                field = field.reshape(4, 4, 8, 256)
                for g in range(4):
                    j = c * 4 + lax.rem(g + 4 - mem, 4)
                    weights = pert[j, pl.ds(kg * 4, 4), :, cols].astype(F32)
                    part = jnp.sum(field[g] * weights, axis=0)
                    if step:
                        part = part + total[g, :, cols]
                    if step == 3:
                        out[j, :, cols] = part.astype(BF16)
                    else:
                        total[g, :, cols] = part
        pltpu.make_async_copy(
            snd.at[c, pl.ds(0, 255)], snd.at[c, pl.ds(0, 255)], send_sem.at[c]
        ).wait()
        return 0

    lax.fori_loop(0, 3, finish, 0)


def shards(control, vert_root, loc_spec, legendre, wave_table, lat_order, perturb):
    hbm = pl.BlockSpec(memory_space=pl.ANY)
    return pl.pallas_call(
        kernel,
        name="synthesis",
        out_shape=pltpu.VMEM((12, 8, 1536), BF16),
        in_specs=[hbm] * 7,
        out_specs=pl.BlockSpec(memory_space=pltpu.VMEM),
        scratch_shapes=[
            pltpu.VMEM((32, 32), F32),
            pltpu.VMEM((1, 512), F32),
            pltpu.VMEM((4, 128), jnp.int32),
            pltpu.VMEM((6, 128), jnp.int32),
            pltpu.VMEM((4, 32, 2, 8, 512), BF16),
            pltpu.VMEM((8, 512, 768), BF16),
            pltpu.VMEM((12, 16, 8, 1536), BF16),
            pltpu.VMEM((4, 4, 4, 8, 512), F32),
            pltpu.VMEM((4, 256, 512), BF16),
            pltpu.VMEM((8, 256, 768), BF16),
            pltpu.VMEM((768, 128), F32),
            pltpu.VMEM((2, 256, 256), BF16),
            pltpu.VMEM((256, 768), BF16),
            pltpu.VMEM((64 * 72, 128), F32),
            pltpu.VMEM((3, 256, 2, 8, 128), BF16),
            pltpu.VMEM((3, 256, 2, 8, 128), BF16),
            pltpu.VMEM((1024, 128), F32),
            pltpu.VMEM((1024, 1536), BF16),
            pltpu.VMEM((128, 1024), BF16),
            pltpu.VMEM((4, 8, 1536), F32),
            pltpu.SemaphoreType.DMA((5,)),
            pltpu.SemaphoreType.DMA((8,)),
            pltpu.SemaphoreType.DMA((4,)),
            pltpu.SemaphoreType.DMA((3,)),
            pltpu.SemaphoreType.DMA((3, 4)),
        ],
        compiler_params=pltpu.CompilerParams(
            collective_id=0, has_side_effects=True, vmem_limit_bytes=60 * 1024 * 1024
        ),
    )(
        control, vert_root, loc_spec.reshape(1, 512), legendre,
        wave_table.reshape(4, 128), lat_order.reshape(6, 128), perturb,
    )


def solution(mesh):
    return jax.shard_map(
        shards,
        mesh=mesh,
        in_specs=(
            P("mem", None, None, "rows", None),
            P(),
            P(),
            P("rows", None, None),
            P(),
            P(),
            P("rows", None, "mem", None),
        ),
        out_specs=P("rows", "mem", None),
        check_vma=False,
    )
```
